256 devices in a mesh: gx: 16 (over y_hi, z), gy: 16 (over x, y_lo, core).
Axes of the slice: x: 4, y: 4 (y_hi: 2, y_lo: 2; y = y_hi * 2 + y_lo), z: 8, core: 2. Of those that a mesh axis runs over, the one named last changes fastest.
Arguments:
- tokens: bfloat16 [256, 8192], P('gy', 'gx'), may hold values from -6 to 6
- target: bfloat16 [256, 8192], P('gy', 'gx'), may hold values from -6 to 6
- w_gate: bfloat16 [8192, 14336], P('gx', 'gy'), may hold values from -0.0625 to 0.0625
- w_up: bfloat16 [8192, 14336], P('gx', 'gy'), may hold values from -0.0625 to 0.0625
- w_down: bfloat16 [14336, 8192], P('gy', 'gx'), may hold values from -0.046875 to 0.046875
- t_gate: bfloat16 [8192, 14336], P('gx', 'gy'), may hold values from -0.0625 to 0.0625
- t_up: bfloat16 [8192, 14336], P('gx', 'gy'), may hold values from -0.0625 to 0.0625
- t_down: bfloat16 [14336, 8192], P('gy', 'gx'), may hold values from -0.046875 to 0.046875
Outputs:
- hvp_gate: bfloat16 [8192, 14336], P('gx', 'gy')
- hvp_up: bfloat16 [8192, 14336], P('gx', 'gy')
- hvp_down: bfloat16 [14336, 8192], P('gy', 'gx')
The draws below stay inside these ranges and needn't reach their ends.
All inputs are finite; a program needn't handle non-finite values.
Results may differ from the reference program's by a relative error of at most 0.0074.
Values may be sent and summed in bfloat16 or wider, within the bound.
A program may use at most 64 MiB of HBM per device.

```python
import math
import jax
import jax.numpy as jnp

D = 8192
FF = 14336
TOKENS = 256


def spiked(drawn, rng, source, target, blocks, factor):
    def block_of(position):
        return (jnp.arange(drawn.shape[position]) // (drawn.shape[position] // blocks)).reshape((-1,) + (1,) * (drawn.ndim - 1 - position))

    near = jax.random.permutation(rng, blocks)[block_of(target)]
    other_side = (block_of(target) + blocks // 2) % blocks
    return jnp.where((block_of(source) == near) | (block_of(source) == other_side), factor * drawn, drawn)


def levels(rng, extent, split, smallest, high):
    factor_of = 1.0
    for axis_at, parts in split:
        draws = jax.random.uniform(jax.random.fold_in(jax.random.fold_in(rng, 6), axis_at), (parts,), jnp.float32, smallest / len(split), high / len(split))
        factor_of = factor_of * jnp.repeat(jnp.exp(draws), extent[axis_at] // parts).reshape((-1,) + (1,) * (len(extent) - 1 - axis_at))
    return factor_of


def centred(own_key, extent, deviation, most, split=(), held_as=jnp.bfloat16):
    loudness = levels(own_key, extent, split, -0.22, 0.18) if split else 1.0
    result = jax.random.normal(own_key, extent, jnp.float32) * deviation * loudness
    return jnp.minimum(jnp.maximum(result, -most), most).astype(held_as)


def heavy_noise(stream_key, shape, spread, limit, shards, heavy, kind=jnp.bfloat16):
    array = spread * jax.random.normal(stream_key, shape, jnp.float32)
    if shards:
        array = array * levels(stream_key, shape, shards, -0.22, 0.18)
    return jnp.clip(spiked(array, jax.random.fold_in(stream_key, 3), *heavy), -limit, limit).astype(kind)


def setup_inputs(seed: int = 0) -> dict:
    key_of = jax.random.split(jax.random.key(seed), 9)
    tokens = heavy_noise(key_of[0], (TOKENS, D), 1.0, 6.0, ((0, 16), (1, 16)), (1, 0, 16, 2.0))
    target = centred(key_of[1], (TOKENS, D), 1.0, 6.0, ((0, 16), (1, 16)))
    w_gate = centred(key_of[2], (D, FF), D ** -0.5, 0.0625, ((0, 16), (1, 16)))
    w_up = centred(key_of[3], (D, FF), D ** -0.5, 0.0625, ((0, 16), (1, 16)))
    w_down = centred(key_of[4], (FF, D), FF ** -0.5, 0.046875, ((0, 16), (1, 16)))
    t_gate = centred(key_of[5], (D, FF), D ** -0.5, 0.0625, ((0, 16), (1, 16)))
    t_up = centred(key_of[6], (D, FF), D ** -0.5, 0.0625, ((0, 16), (1, 16)))
    t_down = centred(key_of[7], (FF, D), FF ** -0.5, 0.046875, ((0, 16), (1, 16)))
    return {"tokens": tokens, "target": target, "w_gate": w_gate, "w_up": w_up, "w_down": w_down, "t_gate": t_gate, "t_up": t_up, "t_down": t_down}


def silu_parts(gate):
    sig = jax.nn.sigmoid(gate)
    first = sig * (1.0 + gate * (1.0 - sig))
    second = sig * (1.0 - sig) * (2.0 + gate * (1.0 - 2.0 * sig))
    return (gate * sig, first, second)

def matmul(left, right):
    return jnp.dot(left, right, preferred_element_type=jnp.float32)

def reference(tokens, target, w_gate, w_up, w_down, t_gate, t_up, t_down):
    scale = 1.0 / math.sqrt(TOKENS)
    gate = matmul(tokens, w_gate)
    upper = matmul(tokens, w_up)
    gate_dot = matmul(tokens, t_gate)
    upper_dot = matmul(tokens, t_up)
    silu_val, first, second = silu_parts(gate)
    hidden = (silu_val * upper).astype(jnp.bfloat16)
    hidden_dot = (first * gate_dot * upper + silu_val * upper_dot).astype(jnp.bfloat16)
    output = matmul(hidden, w_down)
    output_dot = matmul(hidden_dot, w_down) + matmul(hidden, t_down)
    grad = ((output - target.astype(jnp.float32)) * scale).astype(jnp.bfloat16)
    grad_dot = (output_dot * scale).astype(jnp.bfloat16)
    hvp_down = (matmul(hidden_dot.T, grad) + matmul(hidden.T, grad_dot)).astype(jnp.bfloat16)
    back = matmul(grad, w_down.T)
    back_dot = matmul(grad_dot, w_down.T) + matmul(grad, t_down.T)
    gate_in = (back_dot * upper * first + back * upper_dot * first + back * upper * second * gate_dot).astype(jnp.bfloat16)
    upper_in = (back_dot * silu_val + back * first * gate_dot).astype(jnp.bfloat16)
    hvp_gate = matmul(tokens.T, gate_in).astype(jnp.bfloat16)
    hvp_up = matmul(tokens.T, upper_in).astype(jnp.bfloat16)
    return (hvp_gate, hvp_up, hvp_down)
```

```python
import functools
import math

import jax
import jax.numpy as jnp
from jax import lax
from jax.experimental import pallas as pl
from jax.experimental.pallas import tpu as pltpu
from jax.sharding import PartitionSpec as P

MESH = pl.DeviceIdType.MESH
TOKENS = 256
DL = 512
FL = 896
NZ = 8
NG = 16
ROWS = 32
F32 = jnp.float32
BF16 = jnp.bfloat16


def silu_parts(gate):
    sig = jax.nn.sigmoid(gate)
    first = sig * (1.0 + gate * (1.0 - sig))
    second = sig * (1.0 - sig) * (2.0 + gate * (1.0 - 2.0 * sig))
    return (gate * sig, first, second)


def lead_dot(left, right):
    return lax.dot_general(left, right, (((0,), (0,)), ((), ())), preferred_element_type=F32)


def tail_dot(left, right):
    return lax.dot_general(left, right, (((1,), (1,)), ((), ())), preferred_element_type=F32)


def kernel(
    tok, tgt, wg, wu, wd, tg, tu, td,
    x_out, ag_out, g_out,
    xs, tgv, wup, wdn, part, sbuf, rbuf, ysend, yrecv, act, ag, osum, osend, orecv, gs,
    lsem, p0s, p0r, rss, rsr, ys, yr, ags, agr, p3s, p3r, p4s, p4r,
):
    scale = 1.0 / math.sqrt(TOKENS)
    g = lax.axis_index("gx")
    h = lax.axis_index("gy")
    yh = lax.div(g, NZ)
    z = lax.rem(g, NZ)
    up_z = yh * NZ + lax.rem(z + 1, NZ)
    dn_z = yh * NZ + lax.rem(z + NZ - 1, NZ)
    pair = lax.rem(g + NZ, 2 * NZ)

    def at_gx(i):
        return {"gx": i}

    def at_gy(i):
        return {"gy": i}

    pending = []

    def send(src, dst, ssem, rsem, where):
        copy = pltpu.make_async_remote_copy(
            src_ref=src, dst_ref=dst, send_sem=ssem, recv_sem=rsem, device_id=where, device_id_type=MESH
        )
        copy.start()
        pending.append(copy)

    def arrived(dst, ssem, rsem, where):
        pltpu.make_async_remote_copy(
            src_ref=dst, dst_ref=dst, send_sem=ssem, recv_sem=rsem, device_id=where, device_id_type=MESH
        ).wait_recv()

    local = []
    own_tok = pltpu.make_async_copy(tok, xs.at[h], lsem.at[0])
    own_tok.start()
    for i, w in enumerate((wg, wu, tg, tu)):
        c = pltpu.make_async_copy(w, wup.at[i], lsem.at[1 + i])
        c.start()
        local.append(c)
    for i, w in enumerate((wd, td)):
        c = pltpu.make_async_copy(w, wdn.at[i], lsem.at[5 + i])
        c.start()
        local.append(c)
    own_tgt = pltpu.make_async_copy(tgt, tgv, lsem.at[7])
    own_tgt.start()

    barrier = pltpu.get_barrier_semaphore()
    for i in (up_z, dn_z, pair):
        pl.semaphore_signal(barrier, inc=1, device_id=at_gx(i), device_id_type=MESH)
    for k in range(1, NG):
        pl.semaphore_signal(barrier, inc=1, device_id=at_gy(lax.rem(h + k, NG)), device_id_type=MESH)
    pl.semaphore_wait(barrier, 3 + NG - 1)

    order = (8, 7, 9, 6, 10, 5, 11, 4, 12, 3, 13, 2, 14, 1, 15)
    own_tok.wait()
    for k in order:
        send(xs.at[h], xs.at[h], p0s.at[k], p0r.at[k], at_gy(lax.rem(h + k, NG)))
    for k in reversed(order):
        src = lax.rem(h + NG - k, NG)
        arrived(xs.at[src], p0s.at[k], p0r.at[k], at_gy(src))
    x_copy = pltpu.make_async_copy(xs, x_out, lsem.at[8])
    x_copy.start()

    tokens = xs[...].reshape(TOKENS, DL)

    def zrow(i):
        return pl.ds(pl.multiple_of(ROWS * lax.rem(i + NZ, NZ), ROWS), ROWS)

    def long_way(u):
        return u % 2

    def first_step(u, d):
        return 0 if d == long_way(u) else 1

    def rs_send(u, d, s):
        ahead = 4 - s
        row = zrow(z + ahead) if d == 0 else zrow(z - ahead)
        val = part[u, row, :]
        if s > first_step(u, d):
            arrived(rbuf.at[u, d, s - 1], rss.at[u, d, s - 1], rsr.at[u, d, s - 1], at_gx(dn_z if d == 0 else up_z))
            val = val + rbuf[u, d, s - 1].astype(F32)
        sbuf[u, d, s] = val.astype(BF16)
        send(sbuf.at[u, d, s], rbuf.at[u, d, s], rss.at[u, d, s], rsr.at[u, d, s], at_gx(up_z if d == 0 else dn_z))

    def rs_start(u):
        d = long_way(u)
        rs_send(u, d, 0)
        rs_send(u, 1 - d, 1)

    def rs_last(u):
        val = part[u, zrow(z), :]
        for d in range(2):
            arrived(rbuf.at[u, d, 3], rss.at[u, d, 3], rsr.at[u, d, 3], at_gx(dn_z if d == 0 else up_z))
            val = val + rbuf[u, d, 3].astype(F32)
        part[u, zrow(z), :] = val
        ysend[u] = val.astype(BF16)
        send(ysend.at[u], yrecv.at[u], ys.at[u], yr.at[u], at_gx(pair))

    def rs_result(u):
        arrived(yrecv.at[u], ys.at[u], yr.at[u], at_gx(pair))
        return part[u, zrow(z), :] + yrecv[u].astype(F32)

    def rs_middle(units):
        for s in range(1, 4):
            for u in units:
                for d in range(2):
                    if s > first_step(u, d):
                        rs_send(u, d, s)

    def ag_send(v, d, s):
        src = zrow(z - s) if d == 0 else zrow(z + s)
        if s > 0:
            ag_wait(v, d, s - 1)
        send(
            ag.at[v, src, :], ag.at[v, src, :], ags.at[v, d, s], agr.at[v, d, s],
            at_gx(up_z if d == 0 else dn_z),
        )

    def ag_wait(v, d, s):
        src = zrow(z - 1 - s) if d == 0 else zrow(z + 1 + s)
        arrived(ag.at[v, src, :], ags.at[v, d, s], agr.at[v, d, s], at_gx(dn_z if d == 0 else up_z))

    def ag_start(v):
        for d in range(2):
            ag_send(v, d, 0)

    def ag_finish(units):
        for s in range(1, 4):
            for v in units:
                for d in range(2):
                    if s < 3 or d == long_way(v):
                        ag_send(v, d, s)
        for v in units:
            for d in range(2):
                ag_wait(v, d, 3 if d == long_way(v) else 2)

    for u in range(4):
        local[u].wait()
        for n in range(0, FL, 256):
            m = min(256, FL - n)
            part[u, :, n : n + m] = jnp.dot(tokens, wup[u, :, n : n + m], preferred_element_type=F32)
        rs_start(u)
    rs_middle(range(4))
    for u in range(4):
        rs_last(u)
    gate, upper = rs_result(0), rs_result(1)
    silu_val, first, second = silu_parts(gate)
    ag[0, zrow(z), :] = (silu_val * upper).astype(BF16)
    ag_start(0)
    gate_dot, upper_dot = rs_result(2), rs_result(3)
    ag[1, zrow(z), :] = (first * gate_dot * upper + silu_val * upper_dot).astype(BF16)
    ag_start(1)
    act[0] = gate
    act[1] = upper
    act[2] = gate_dot
    act[3] = upper_dot
    for c in local[4:]:
        c.wait()
    ag_finish((0, 1))

    def out_send(w):
        for k in order:
            dst = lax.rem(h + k, NG)
            send(osend.at[w, dst], orecv.at[w, k], p3s.at[w, k], p3r.at[w, k], at_gy(dst))

    def out_sum(w):
        total = osum[w, h]
        for k in reversed(order):
            arrived(orecv.at[w, k], p3s.at[w, k], p3r.at[w, k], at_gy(lax.rem(h + NG - k, NG)))
            total = total + orecv[w, k].astype(F32)
        return total

    def grad_send(w):
        for k in order:
            send(gs.at[w, h], gs.at[w, h], p4s.at[w, k], p4r.at[w, k], at_gy(lax.rem(h + k, NG)))

    def grad_wait(w):
        for k in reversed(order):
            src = lax.rem(h + NG - k, NG)
            arrived(gs.at[w, src], p4s.at[w, k], p4r.at[w, k], at_gy(src))

    for w in range(2):
        for n in range(0, DL, 256):
            if w == 0:
                val = jnp.dot(ag[0], wdn[0, :, n : n + 256], preferred_element_type=F32)
            else:
                val = jnp.dot(ag[1], wdn[0, :, n : n + 256], preferred_element_type=F32)
                val = val + jnp.dot(ag[0], wdn[1, :, n : n + 256], preferred_element_type=F32)
            val = val.reshape(NG, TOKENS // NG, 256)
            osum[w, :, :, n : n + 256] = val
            osend[w, :, :, n : n + 256] = val.astype(BF16)
        out_send(w)
    own_tgt.wait()
    gs[0, h] = ((out_sum(0) - tgv[...].astype(F32)) * scale).astype(BF16)
    grad_send(0)
    gs[1, h] = (out_sum(1) * scale).astype(BF16)
    grad_send(1)

    def back_part(w):
        for n in range(0, FL, 256):
            m = min(256, FL - n)
            if w == 0:
                val = tail_dot(gs[0].reshape(TOKENS, DL), wdn[0, n : n + m, :])
            else:
                val = tail_dot(gs[1].reshape(TOKENS, DL), wdn[0, n : n + m, :])
                val = val + tail_dot(gs[0].reshape(TOKENS, DL), wdn[1, n : n + m, :])
            part[4 + w, :, n : n + m] = val

    for w in range(2):
        grad_wait(w)
        back_part(w)
        rs_start(4 + w)
    rs_middle((4, 5))
    g_copy = pltpu.make_async_copy(gs, g_out, lsem.at[9])
    g_copy.start()
    for u in (4, 5):
        rs_last(u)
    gate, upper, gate_dot, upper_dot = act[0], act[1], act[2], act[3]
    silu_val, first, second = silu_parts(gate)
    back = rs_result(4)
    back_dot = rs_result(5)
    ag[2, zrow(z), :] = (
        back_dot * upper * first + back * upper_dot * first + back * upper * second * gate_dot
    ).astype(BF16)
    ag_start(2)
    ag[3, zrow(z), :] = (back_dot * silu_val + back * first * gate_dot).astype(BF16)
    ag_start(3)
    ag_finish((2, 3))
    ag_copy = pltpu.make_async_copy(ag, ag_out, lsem.at[10])
    ag_copy.start()
    for c in pending:
        c.wait_send()
    x_copy.wait()
    g_copy.wait()
    ag_copy.wait()


def body(tokens, target, w_gate, w_up, w_down, t_gate, t_up, t_down):
    any_spec = pl.BlockSpec(memory_space=pl.ANY)
    blk = TOKENS // NG
    dma = pltpu.SemaphoreType.DMA
    xfull, ag, gs = pl.pallas_call(
        kernel,
        out_shape=(
            jax.ShapeDtypeStruct((NG, blk, DL), BF16),
            jax.ShapeDtypeStruct((4, TOKENS, FL), BF16),
            jax.ShapeDtypeStruct((2, NG, blk, DL), BF16),
        ),
        in_specs=[any_spec] * 8,
        out_specs=(any_spec,) * 3,
        scratch_shapes=[
            pltpu.VMEM((NG, blk, DL), BF16),
            pltpu.VMEM((blk, DL), BF16),
            pltpu.VMEM((4, DL, FL), BF16),
            pltpu.VMEM((2, FL, DL), BF16),
            pltpu.VMEM((6, TOKENS, FL), F32),
            pltpu.VMEM((6, 2, 4, ROWS, FL), BF16),
            pltpu.VMEM((6, 2, 4, ROWS, FL), BF16),
            pltpu.VMEM((6, ROWS, FL), BF16),
            pltpu.VMEM((6, ROWS, FL), BF16),
            pltpu.VMEM((4, ROWS, FL), F32),
            pltpu.VMEM((4, TOKENS, FL), BF16),
            pltpu.VMEM((2, NG, blk, DL), F32),
            pltpu.VMEM((2, NG, blk, DL), BF16),
            pltpu.VMEM((2, NG, blk, DL), BF16),
            pltpu.VMEM((2, NG, blk, DL), BF16),
            dma((11,)),
            dma((NG,)), dma((NG,)),
            dma((6, 2, 4)), dma((6, 2, 4)),
            dma((6,)), dma((6,)),
            dma((4, 2, 4)), dma((4, 2, 4)),
            dma((2, NG)), dma((2, NG)),
            dma((2, NG)), dma((2, NG)),
        ],
        compiler_params=pltpu.CompilerParams(
            collective_id=0, has_side_effects=True, vmem_limit_bytes=40 * 1024 * 1024
        ),
    )(tokens, target, w_gate, w_up, w_down, t_gate, t_up, t_down)
    xfull = xfull.reshape(TOKENS, DL)
    gs = gs.reshape(2, TOKENS, DL)
    hvp_down = (lead_dot(ag[1], gs[0]) + lead_dot(ag[0], gs[1])).astype(BF16)
    hvp_gate = lead_dot(xfull, ag[2]).astype(BF16)
    hvp_up = lead_dot(xfull, ag[3]).astype(BF16)
    return (hvp_gate, hvp_up, hvp_down)


def solution(mesh):
    in_specs = (
        P("gy", "gx"),
        P("gy", "gx"),
        P("gx", "gy"),
        P("gx", "gy"),
        P("gy", "gx"),
        P("gx", "gy"),
        P("gx", "gy"),
        P("gy", "gx"),
    )
    out_specs = (P("gx", "gy"), P("gx", "gy"), P("gy", "gx"))
    return jax.shard_map(body, mesh=mesh, in_specs=in_specs, out_specs=out_specs, check_vma=False)
```

```python
import functools
import math

import jax
import jax.numpy as jnp
from jax import lax
from jax.experimental import pallas as pl
from jax.experimental.pallas import tpu as pltpu
from jax.sharding import PartitionSpec as P

MESH = pl.DeviceIdType.MESH
TOKENS = 256
DL = 512
FL = 896
NZ = 8
NG = 16
ROWS = 32
F32 = jnp.float32
BF16 = jnp.bfloat16


def silu_parts(gate):
    sig = jax.nn.sigmoid(gate)
    first = sig * (1.0 + gate * (1.0 - sig))
    second = sig * (1.0 - sig) * (2.0 + gate * (1.0 - 2.0 * sig))
    return (gate * sig, first, second)


def lead_dot(left, right):
    return lax.dot_general(left, right, (((0,), (0,)), ((), ())), preferred_element_type=F32)


def tail_dot(left, right):
    return lax.dot_general(left, right, (((1,), (1,)), ((), ())), preferred_element_type=F32)


def encode2(v):
    return (v * jnp.abs(v)).astype(BF16)


def decode2(c):
    v = c.astype(F32)
    root = jnp.sqrt(jnp.abs(v))
    return jnp.where(v < 0.0, -root, root)


def encode4(v):
    return (v * jnp.abs(v) * (v * v)).astype(BF16)


def decode4(c):
    v = c.astype(F32)
    root = jnp.sqrt(jnp.sqrt(jnp.abs(v)))
    return jnp.where(v < 0.0, -root, root)


def kernel(
    tok, tgt, wg, wu, wd, tg, tu, td,
    xt_out, ag_out, hd_out,
    xs, tgv, wup, wdn, part, sbuf, rbuf, ysend, yrecv, act, ag, osum, osend, ocore, orecv, gs,
    lsem, p0s, p0r, rss, rsr, ys, yr, ags, agr, p3s, p3r, p4s, p4r, ds, dr,
):
    scale = 1.0 / math.sqrt(TOKENS)
    g = lax.axis_index("gx")
    h = lax.axis_index("gy")
    core = lax.rem(h, 2)
    mine = lax.div(h, 2)
    mate = h + 1 - 2 * core
    yh = lax.div(g, NZ)
    z = lax.rem(g, NZ)
    up_z = yh * NZ + lax.rem(z + 1, NZ)
    dn_z = yh * NZ + lax.rem(z + NZ - 1, NZ)
    pair = lax.rem(g + NZ, 2 * NZ)

    def at_gx(i):
        return {"gx": i}

    def at_gy(i):
        return {"gy": i}

    pending = []

    def enc(u, v):
        return encode4(v) if u < 4 else encode2(v)

    def dec(u, v):
        return decode4(v) if u < 4 else decode2(v)

    def send(src, dst, ssem, rsem, where):
        copy = pltpu.make_async_remote_copy(
            src_ref=src, dst_ref=dst, send_sem=ssem, recv_sem=rsem, device_id=where, device_id_type=MESH
        )
        copy.start()
        pending.append(copy)

    def arrived(dst, ssem, rsem, where):
        pltpu.make_async_remote_copy(
            src_ref=dst, dst_ref=dst, send_sem=ssem, recv_sem=rsem, device_id=where, device_id_type=MESH
        ).wait_recv()

    far = (4, 5, 3, 6, 2, 7, 1)

    def spread(ref, ssem, rsem):
        for k in far:
            send(ref.at[h], ref.at[h], ssem.at[k], rsem.at[k], at_gy(lax.rem(h + 2 * k, NG)))
        send(ref.at[h], ref.at[h], ssem.at[8], rsem.at[8], at_gy(mate))

    def collect(ref, ssem, rsem):
        for k in reversed(far):
            src = lax.rem(h + NG - 2 * k, NG)
            arrived(ref.at[src], ssem.at[k], rsem.at[k], at_gy(src))
            send(ref.at[src], ref.at[src], ssem.at[8 + k], rsem.at[8 + k], at_gy(mate))
        arrived(ref.at[mate], ssem.at[8], rsem.at[8], at_gy(mate))
        for k in reversed(far):
            src = lax.rem(mate + NG - 2 * k, NG)
            arrived(ref.at[src], ssem.at[8 + k], rsem.at[8 + k], at_gy(mate))

    local = []
    own_tok = pltpu.make_async_copy(tok, xs.at[h], lsem.at[0])
    own_tok.start()
    for i, w in enumerate((wg, wu, tg, tu)):
        c = pltpu.make_async_copy(w, wup.at[i], lsem.at[1 + i])
        c.start()
        local.append(c)
    for i, w in enumerate((wd, td)):
        c = pltpu.make_async_copy(w, wdn.at[i], lsem.at[5 + i])
        c.start()
        local.append(c)
    own_tgt = pltpu.make_async_copy(tgt, tgv, lsem.at[7])
    own_tgt.start()

    barrier = pltpu.get_barrier_semaphore()
    for i in (up_z, dn_z, pair):
        pl.semaphore_signal(barrier, inc=1, device_id=at_gx(i), device_id_type=MESH)
    for k in range(1, 8):
        pl.semaphore_signal(barrier, inc=1, device_id=at_gy(lax.rem(h + 2 * k, NG)), device_id_type=MESH)
    pl.semaphore_signal(barrier, inc=1, device_id=at_gy(mate), device_id_type=MESH)
    pl.semaphore_wait(barrier, 11)

    own_tok.wait()
    spread(xs, p0s, p0r)
    collect(xs, p0s, p0r)

    tokens = xs[...].reshape(TOKENS, DL)

    def zrow(i):
        return pl.ds(pl.multiple_of(ROWS * lax.rem(i + NZ, NZ), ROWS), ROWS)

    def long_way(u):
        return u % 2

    def first_step(u, d):
        return 0 if d == long_way(u) else 1

    def rs_send(u, d, s):
        ahead = 4 - s
        row = zrow(z + ahead) if d == 0 else zrow(z - ahead)
        val = part[u, row, :]
        if s > first_step(u, d):
            arrived(rbuf.at[u, d, s - 1], rss.at[u, d, s - 1], rsr.at[u, d, s - 1], at_gx(dn_z if d == 0 else up_z))
            val = val + dec(u, rbuf[u, d, s - 1])
        sbuf[u, d, s] = enc(u, val)
        send(sbuf.at[u, d, s], rbuf.at[u, d, s], rss.at[u, d, s], rsr.at[u, d, s], at_gx(up_z if d == 0 else dn_z))

    def rs_start(u):
        d = long_way(u)
        rs_send(u, d, 0)
        rs_send(u, 1 - d, 1)

    def rs_last(u):
        val = part[u, zrow(z), :]
        for d in range(2):
            arrived(rbuf.at[u, d, 3], rss.at[u, d, 3], rsr.at[u, d, 3], at_gx(dn_z if d == 0 else up_z))
            val = val + dec(u, rbuf[u, d, 3])
        part[u, zrow(z), :] = val
        ysend[u] = enc(u, val)
        send(ysend.at[u], yrecv.at[u], ys.at[u], yr.at[u], at_gx(pair))

    def rs_result(u):
        arrived(yrecv.at[u], ys.at[u], yr.at[u], at_gx(pair))
        return part[u, zrow(z), :] + dec(u, yrecv[u])

    def rs_middle(units):
        for s in range(1, 4):
            for u in units:
                for d in range(2):
                    if s > first_step(u, d):
                        rs_send(u, d, s)

    def ag_send(v, d, s):
        src = zrow(z - s) if d == 0 else zrow(z + s)
        if s > 0:
            ag_wait(v, d, s - 1)
        send(
            ag.at[v, src, :], ag.at[v, src, :], ags.at[v, d, s], agr.at[v, d, s],
            at_gx(up_z if d == 0 else dn_z),
        )

    def ag_wait(v, d, s):
        src = zrow(z - 1 - s) if d == 0 else zrow(z + 1 + s)
        arrived(ag.at[v, src, :], ags.at[v, d, s], agr.at[v, d, s], at_gx(dn_z if d == 0 else up_z))

    def ag_start(v):
        for d in range(2):
            ag_send(v, d, 0)

    def ag_finish(units):
        for s in range(1, 4):
            for v in units:
                for d in range(2):
                    if s < 3 or d == long_way(v):
                        ag_send(v, d, s)
        for v in units:
            for d in range(2):
                ag_wait(v, d, 3 if d == long_way(v) else 2)

    for u in range(4):
        local[u].wait()
        for n in range(0, FL, 256):
            m = min(256, FL - n)
            part[u, :, n : n + m] = jnp.dot(tokens, wup[u, :, n : n + m], preferred_element_type=F32)
        rs_start(u)
    xt_out[...] = tokens.T
    rs_middle(range(4))
    for u in range(4):
        rs_last(u)
    gate, upper = rs_result(0), rs_result(1)
    silu_val, first, second = silu_parts(gate)
    ag[0, zrow(z), :] = (silu_val * upper).astype(BF16)
    ag_start(0)
    gate_dot, upper_dot = rs_result(2), rs_result(3)
    ag[1, zrow(z), :] = (first * gate_dot * upper + silu_val * upper_dot).astype(BF16)
    ag_start(1)
    act[0] = gate
    act[1] = upper
    act[2] = gate_dot
    act[3] = upper_dot
    for c in local[4:]:
        c.wait()
    ag_finish((0, 1))

    def out_part(w):
        for n in range(0, DL, 256):
            if w == 0:
                val = jnp.dot(ag[0], wdn[0, :, n : n + 256], preferred_element_type=F32)
            else:
                val = jnp.dot(ag[1], wdn[0, :, n : n + 256], preferred_element_type=F32)
                val = val + jnp.dot(ag[0], wdn[1, :, n : n + 256], preferred_element_type=F32)
            osum[w, :, :, :, n : n + 256] = val.reshape(8, 2, TOKENS // NG, 256)
        osend[w, 0] = encode2(osum[w, :, 1 - core])
        send(osend.at[w, 0], ocore.at[w], ds.at[w], dr.at[w], at_gy(mate))

    def out_send(w):
        arrived(ocore.at[w], ds.at[w], dr.at[w], at_gy(mate))
        for k in far:
            dst = lax.rem(mine + k, 8)
            osend[w, 1, k] = encode2(osum[w, dst, core] + decode2(ocore[w, dst]))
            send(osend.at[w, 1, k], orecv.at[w, k], p3s.at[w, k], p3r.at[w, k], at_gy(2 * dst + core))

    def out_sum(w):
        total = osum[w, mine, core] + decode2(ocore[w, mine])
        for k in reversed(far):
            arrived(orecv.at[w, k], p3s.at[w, k], p3r.at[w, k], at_gy(lax.rem(h + NG - 2 * k, NG)))
            total = total + decode2(orecv[w, k])
        return total

    out_part(0)
    out_part(1)
    out_send(0)
    out_send(1)
    own_tgt.wait()
    gs[0, h] = ((out_sum(0) - tgv[...].astype(F32)) * scale).astype(BF16)
    spread(gs.at[0], p4s.at[0], p4r.at[0])
    gs[1, h] = (out_sum(1) * scale).astype(BF16)
    spread(gs.at[1], p4s.at[1], p4r.at[1])

    def back_part(w):
        for n in range(0, FL, 256):
            m = min(256, FL - n)
            if w == 0:
                val = tail_dot(gs[0].reshape(TOKENS, DL), wdn[0, n : n + m, :])
            else:
                val = tail_dot(gs[1].reshape(TOKENS, DL), wdn[0, n : n + m, :])
                val = val + tail_dot(gs[0].reshape(TOKENS, DL), wdn[1, n : n + m, :])
            part[4 + w, :, n : n + m] = val

    def down_part(n):
        g0 = gs[0, :, :, n : n + 256].reshape(TOKENS, 256)
        g1 = gs[1, :, :, n : n + 256].reshape(TOKENS, 256)
        hd_out[:, n : n + 256] = (lead_dot(ag[1], g0) + lead_dot(ag[0], g1)).astype(BF16)

    for w in range(2):
        collect(gs.at[w], p4s.at[w], p4r.at[w])
        back_part(w)
        rs_start(4 + w)
    down_part(0)
    rs_middle((4, 5))
    for u in (4, 5):
        rs_last(u)
    gate, upper, gate_dot, upper_dot = act[0], act[1], act[2], act[3]
    silu_val, first, second = silu_parts(gate)
    back = rs_result(4)
    back_dot = rs_result(5)
    ag[2, zrow(z), :] = (
        back_dot * upper * first + back * upper_dot * first + back * upper * second * gate_dot
    ).astype(BF16)
    ag_start(2)
    ag[3, zrow(z), :] = (back_dot * silu_val + back * first * gate_dot).astype(BF16)
    ag_start(3)
    down_part(256)
    ag_finish((2, 3))
    ag_copy = pltpu.make_async_copy(ag.at[pl.ds(2, 2)], ag_out, lsem.at[8])
    ag_copy.start()
    for c in pending:
        c.wait_send()
    ag_copy.wait()


def weights_kernel(xt, ag, hd, gate_out, up_out, down_out, buf, sem):
    rows = DL // 4
    down = pltpu.make_async_copy(hd, down_out, sem.at[8])
    down.start()
    copies = []
    for v, out in enumerate((gate_out, up_out)):
        for i in range(4):
            part = pl.ds(i * rows, rows)
            buf[v, part, :] = jnp.dot(xt[part, :], ag[v], preferred_element_type=F32).astype(BF16)
            copy = pltpu.make_async_copy(buf.at[v, part, :], out.at[part, :], sem.at[4 * v + i])
            copy.start()
            copies.append(copy)
    down.wait()
    for copy in copies:
        copy.wait()


def body(*args):
    hbm = pl.BlockSpec(memory_space=pltpu.HBM)
    vmem = pl.BlockSpec(memory_space=pltpu.VMEM)
    blk = TOKENS // NG
    dma = pltpu.SemaphoreType.DMA
    args = [pltpu.with_memory_space_constraint(a, pltpu.HBM) for a in args]
    xt, ag, hd = pl.pallas_call(
        kernel,
        out_shape=(
            jax.ShapeDtypeStruct((DL, TOKENS), BF16),
            jax.ShapeDtypeStruct((2, TOKENS, FL), BF16),
            jax.ShapeDtypeStruct((FL, DL), BF16),
        ),
        in_specs=[hbm] * 8,
        out_specs=(vmem, pl.BlockSpec(memory_space=pl.ANY), vmem),
        scratch_shapes=[
            pltpu.VMEM((NG, blk, DL), BF16),
            pltpu.VMEM((blk, DL), BF16),
            pltpu.VMEM((4, DL, FL), BF16),
            pltpu.VMEM((2, FL, DL), BF16),
            pltpu.VMEM((6, TOKENS, FL), F32),
            pltpu.VMEM((6, 2, 4, ROWS, FL), BF16),
            pltpu.VMEM((6, 2, 4, ROWS, FL), BF16),
            pltpu.VMEM((6, ROWS, FL), BF16),
            pltpu.VMEM((6, ROWS, FL), BF16),
            pltpu.VMEM((4, ROWS, FL), F32),
            pltpu.VMEM((4, TOKENS, FL), BF16),
            pltpu.VMEM((2, 8, 2, blk, DL), F32),
            pltpu.VMEM((2, 2, 8, blk, DL), BF16),
            pltpu.VMEM((2, 8, blk, DL), BF16),
            pltpu.VMEM((2, 8, blk, DL), BF16),
            pltpu.VMEM((2, NG, blk, DL), BF16),
            dma((9,)),
            dma((NG,)), dma((NG,)),
            dma((6, 2, 4)), dma((6, 2, 4)),
            dma((6,)), dma((6,)),
            dma((4, 2, 4)), dma((4, 2, 4)),
            dma((2, 8)), dma((2, 8)),
            dma((2, NG)), dma((2, NG)),
            dma((2,)), dma((2,)),
        ],
        compiler_params=pltpu.CompilerParams(
            collective_id=0, has_side_effects=True, vmem_limit_bytes=40 * 1024 * 1024
        ),
    )(*args)
    return pl.pallas_call(
        weights_kernel,
        out_shape=(
            jax.ShapeDtypeStruct((DL, FL), BF16),
            jax.ShapeDtypeStruct((DL, FL), BF16),
            jax.ShapeDtypeStruct((FL, DL), BF16),
        ),
        in_specs=[vmem] * 3,
        out_specs=(hbm,) * 3,
        scratch_shapes=[pltpu.VMEM((2, DL, FL), BF16), dma((9,))],
        compiler_params=pltpu.CompilerParams(vmem_limit_bytes=16 * 1024 * 1024),
    )(xt, ag, hd)


def solution(mesh):
    in_specs = (
        P("gy", "gx"),
        P("gy", "gx"),
        P("gx", "gy"),
        P("gx", "gy"),
        P("gy", "gx"),
        P("gx", "gy"),
        P("gx", "gy"),
        P("gy", "gx"),
    )
    out_specs = (P("gx", "gy"), P("gx", "gy"), P("gy", "gx"))
    return jax.shard_map(body, mesh=mesh, in_specs=in_specs, out_specs=out_specs, check_vma=False)
```

```python
import functools
import math

import jax
import jax.numpy as jnp
from jax import lax
from jax.experimental import pallas as pl
from jax.experimental.pallas import tpu as pltpu
from jax.sharding import PartitionSpec as P

MESH = pl.DeviceIdType.MESH
TOKENS = 256
DL = 512
FL = 896
NZ = 8
NG = 16
F32 = jnp.float32
BF16 = jnp.bfloat16


def silu_parts(gate):
    sig = jax.nn.sigmoid(gate)
    first = sig * (1.0 + gate * (1.0 - sig))
    second = sig * (1.0 - sig) * (2.0 + gate * (1.0 - 2.0 * sig))
    return (gate * sig, first, second)


def lead_dot(left, right):
    return lax.dot_general(left, right, (((0,), (0,)), ((), ())), preferred_element_type=F32)


def tail_dot(left, right):
    return lax.dot_general(left, right, (((1,), (1,)), ((), ())), preferred_element_type=F32)


def encode2(v):
    return (v * jnp.abs(v)).astype(BF16)


def decode2(c):
    v = c.astype(F32)
    root = jnp.sqrt(jnp.abs(v))
    return jnp.where(v < 0.0, -root, root)


def encode4(v):
    return (v * jnp.abs(v) * (v * v)).astype(BF16)


def decode4(c):
    v = c.astype(F32)
    root = jnp.sqrt(jnp.sqrt(jnp.abs(v)))
    return jnp.where(v < 0.0, -root, root)


def kernel(
    tok, tgt, wg, wu, wd, tg, tu, td,
    xt_out, ag_out, hd_out,
    xs, xt, hd, tgv, wup, wdn, part, sbuf, rbuf, pbuf, fin, act, ag, osum, osend, ocore, oown, orecv, gs,
    lsem, xsem, rss, pss, rsr, fsr, ags, agr, oss, osr, gss, gsr,
):
    scale = 1.0 / math.sqrt(TOKENS)
    g = lax.axis_index("gx")
    h = lax.axis_index("gy")
    core = lax.rem(h, 2)
    mine = lax.div(h, 2)
    mate = h + 1 - 2 * core
    yh = lax.div(g, NZ)
    z = lax.rem(g, NZ)
    own8 = pl.ds(pl.multiple_of(64 * core + 8 * mine, 8), 8)
    core64 = pl.ds(pl.multiple_of(64 * core, 64), 64)
    zown = pl.ds(pl.multiple_of(16 * z + 8 * yh, 8), 8)

    def zat(k):
        return lax.rem(z + k + NZ, NZ)

    def column(k, other=False):
        y = 1 - yh if other else yh
        return {"gx": y * NZ + zat(k)}

    def at_gy(i):
        return {"gy": i}

    def way(d, k):
        return k if d == 0 else -k

    def send(src, dst, ssem, rsem, where):
        pltpu.make_async_remote_copy(
            src_ref=src, dst_ref=dst, send_sem=ssem, recv_sem=rsem, device_id=where, device_id_type=MESH
        ).start()

    def arrived(ref, sem):
        pltpu.make_async_remote_copy(
            src_ref=ref, dst_ref=ref, send_sem=sem, recv_sem=sem, device_id=at_gy(mate), device_id_type=MESH
        ).wait_recv()

    def left(ref, sem):
        pltpu.make_async_remote_copy(
            src_ref=ref, dst_ref=ref, send_sem=sem, recv_sem=sem, device_id=at_gy(mate), device_id_type=MESH
        ).wait_send()

    def local_copy(src, dst, i):
        copy = pltpu.make_async_copy(src, dst, lsem.at[i])
        copy.start()
        return copy

    own_tok = [local_copy(tok.at[pl.ds(8 * t, 8), :], xs.at[t, own8, :], t) for t in range(2)]
    local = [local_copy(w, wup.at[i], 2 + i) for i, w in enumerate((wg, wu, tg, tu))]
    local += [local_copy(w, wdn.at[i], 6 + i) for i, w in enumerate((wd, td))]
    own_tgt = local_copy(tgt, tgv, 8)

    with jax.named_scope("barrier"):
        barrier = pltpu.get_barrier_semaphore()
        near = [column(k, o) for k in (1, -1, 2, -2) for o in (False, True)] + [column(0, True)]
        near += [at_gy(lax.rem(h + 2 * k, NG)) for k in range(1, 8)] + [at_gy(mate)]
        for where in near:
            pl.semaphore_signal(barrier, inc=1, device_id=where, device_id_type=MESH)
        pl.semaphore_wait(barrier, len(near))

    far = (4, 5, 3, 6, 2, 7, 1)

    def spread(block, ssem, rsem):
        for k in far:
            send(block, block, ssem, rsem, at_gy(lax.rem(h + 2 * k, NG)))

    def hand_on(seven, eight, rsem, dsem, drsem):
        arrived(seven, rsem)
        send(eight, eight, dsem, drsem, at_gy(mate))

    with jax.named_scope("tokens"):
        for c in own_tok:
            c.wait()
        spread(xs.at[:, own8, :], xsem.at[0], xsem.at[1])
        hand_on(xs.at[:, pl.ds(0, 56), :], xs.at[:, core64, :], xsem.at[1], xsem.at[2], xsem.at[3])
        arrived(xs.at[:, pl.ds(0, 64), :], xsem.at[3])

    slots = {}

    def slot_of(tq):
        slots[tq] = slots.get(tq, -1) + 1
        return slots[tq]

    def enc(q, v):
        return encode4(v) if q < 2 else encode2(v)

    def dec(q, v):
        return decode4(v) if q < 2 else decode2(v)

    def long_way(q, t):
        return (q + t) % 2

    def chunk(t, q, d, k):
        return part[t, q, pl.ds(2 * zat(way(d, k)), 2)]

    def send_whole(t, q, val, d, hops, slot):
        tq = 3 * t + q
        i = slot_of(tq)
        sbuf[tq, i] = enc(q, val)
        send(sbuf.at[tq, i], rbuf.at[tq, d, slot], rss, rsr.at[tq, d, slot], column(way(d, hops)))

    def send_last(t, q, val, d, hops, slot):
        tq = 3 * t + q
        i = slot_of(tq)
        sbuf[tq, i] = enc(q, val)
        for other in (True, False):
            y = 1 - yh if other else yh
            dst = fin.at[tq, slot + d + (2 if other else 0)]
            send(sbuf.at[tq, i, y], dst, rss, fsr.at[tq], column(way(d, hops), other))

    def send_pair(t, q):
        tq = 3 * t + q
        pbuf[tq] = enc(q, part[t, q, 2 * z + 1 - yh])
        send(pbuf.at[tq], fin.at[tq, 4], pss, fsr.at[tq], column(0, True))

    def taken(t, q, d, slot):
        tq = 3 * t + q
        arrived(rbuf.at[tq, d, slot], rsr.at[tq, d, slot])
        return dec(q, rbuf[tq, d, slot])

    def total(t, q, n):
        tq = 3 * t + q
        arrived(fin.at[tq, pl.ds(0, n)], fsr.at[tq])
        val = part[t, q, 2 * z + yh]
        for i in range(n):
            val = val + dec(q, fin[tq, i])
        return val

    def up(t, q):
        for u in range(2):
            for n in range(0, FL, 256):
                m = min(256, FL - n)
                val = jnp.dot(xs[t], wup[2 * q + u, :, n : n + m], preferred_element_type=F32)
                part[t, q, :, u, :, n : n + m] = val.reshape(16, 8, m)
        d = long_way(q, t)
        send_whole(t, q, chunk(t, q, d, 4), d, 1, 0)
        send_whole(t, q, chunk(t, q, 1 - d, 3), 1 - d, 1, 1)
        send_pair(t, q)

    def ring(t, q, d, s):
        val = chunk(t, q, d, 4 - s) + taken(t, q, d, s - 1)
        if s < 3:
            send_whole(t, q, val, d, 1, s)
        else:
            send_last(t, q, val, d, 1, 0)

    def gather(v, t):
        own = ag.at[v, :, t, zown, :]
        for d in range(2):
            for other in (True, False):
                send(own, own, ags, agr.at[t, v, d], column(way(d, 2), other))
        for d in range(2):
            for other in (True, False):
                send(own, own, ags, agr.at[t, v, 2], column(way(d, 1), other))
        send(own, own, ags, agr.at[t, v, 2], column(0, True))

    def relay(v, t, d):
        arrived(ag.at[v, :, t, pl.ds(0, 16), :], agr.at[t, v, d])
        rows = ag.at[v, :, t, pl.ds(pl.multiple_of(16 * zat(way(d, -2)), 16), 16), :]
        if d == long_way(v, t):
            send(rows, rows, ags, agr.at[t, v, 2], column(way(d, 2)))
        send(rows, rows, ags, agr.at[t, v, 2], column(way(d, 1)))

    def gathered(v, t):
        arrived(ag.at[v, :, t, pl.ds(0, 88), :], agr.at[t, v, 2])

    def hidden(t):
        val = total(t, 0, 5)
        gate, upper = val[0], val[1]
        val = total(t, 1, 5)
        gate_dot, upper_dot = val[0], val[1]
        silu_val, first, second = silu_parts(gate)
        ag[0, 0, t, zown, :] = (silu_val * upper).astype(BF16)
        ag[0, 1, t, zown, :] = (first * gate_dot * upper + silu_val * upper_dot).astype(BF16)
        gather(0, t)
        for i, a in enumerate((gate, upper, gate_dot, upper_dot)):
            act[t, i] = a

    def out(t):
        gathered(0, t)
        for n in range(0, DL, 256):
            cols = slice(n, n + 256)
            val = jnp.dot(ag[0, 0, t], wdn[0, :, cols], preferred_element_type=F32)
            osum[t, :, :, 0, :, cols] = val.reshape(2, 8, 8, 256)
            val = jnp.dot(ag[0, 1, t], wdn[0, :, cols], preferred_element_type=F32)
            val = val + jnp.dot(ag[0, 0, t], wdn[1, :, cols], preferred_element_type=F32)
            osum[t, :, :, 1, :, cols] = val.reshape(2, 8, 8, 256)
        osend[t] = encode2(osum[t, 1 - core])
        send(osend.at[t], ocore.at[t], oss.at[0], osr.at[t], at_gy(mate))

    def out_send(t):
        arrived(ocore.at[t], osr.at[t])
        val = osum[t, core] + decode2(ocore[t])
        osum[t, core] = val
        oown[t] = encode2(val)
        for k in far:
            dst = lax.rem(mine + k, 8)
            send(oown.at[t, dst], orecv.at[t, k], oss.at[1], osr.at[2 + t], at_gy(2 * dst + core))

    def grads(t):
        arrived(orecv.at[t, pl.ds(1, 7)], osr.at[2 + t])
        val = osum[t, core, mine]
        for k in range(1, 8):
            val = val + decode2(orecv[t, k])
        target = tgv[8 * t : 8 * t + 8, :].astype(F32)
        gs[t, 0, own8, :] = ((val[0] - target) * scale).astype(BF16)
        gs[t, 1, own8, :] = (val[1] * scale).astype(BF16)
        spread(gs.at[t, :, own8, :], gss.at[0], gsr.at[t])

    def grads_on(t):
        hand_on(gs.at[t, :, pl.ds(0, 56), :], gs.at[t, :, core64, :], gsr.at[t], gss.at[1], gsr.at[2 + t])

    def back(t):
        arrived(gs.at[t, :, pl.ds(0, 64), :], gsr.at[2 + t])
        for n in range(0, FL, 256):
            m = min(256, FL - n)
            val = tail_dot(gs[t, 0], wdn[0, n : n + m, :])
            part[t, 2, :, 0, :, n : n + m] = val.reshape(16, 8, m)
            val = tail_dot(gs[t, 1], wdn[0, n : n + m, :]) + tail_dot(gs[t, 0], wdn[1, n : n + m, :])
            part[t, 2, :, 1, :, n : n + m] = val.reshape(16, 8, m)
        for d in range(2):
            send_whole(t, 2, chunk(t, 2, d, 3), d, 1, 0)
        d = long_way(2, t)
        send_whole(t, 2, chunk(t, 2, d, 4), d, 2, 1)
        for d in range(2):
            send_last(t, 2, chunk(t, 2, d, 1), d, 1, 0)
        send_pair(t, 2)

    def fold(t, d):
        val = chunk(t, 2, d, 2) + taken(t, 2, d, 0)
        if d == long_way(2, t):
            val = val + taken(t, 2, d, 1)
        send_last(t, 2, val, d, 2, 5)

    def inner(t):
        val = total(t, 2, 9)
        back_val, back_dot = val[0], val[1]
        gate, upper, gate_dot, upper_dot = act[t, 0], act[t, 1], act[t, 2], act[t, 3]
        silu_val, first, second = silu_parts(gate)
        ag[1, 0, t, zown, :] = (
            back_dot * upper * first + back_val * upper_dot * first + back_val * upper * second * gate_dot
        ).astype(BF16)
        ag[1, 1, t, zown, :] = (back_dot * silu_val + back_val * first * gate_dot).astype(BF16)
        gather(1, t)

    def down(n):
        g0 = gs[:, 0, :, n : n + 256].reshape(TOKENS, 256)
        g1 = gs[:, 1, :, n : n + 256].reshape(TOKENS, 256)
        hid = ag[0, 0].reshape(TOKENS, FL)
        hid_dot = ag[0, 1].reshape(TOKENS, FL)
        hd[:, n : n + 256] = (lead_dot(hid_dot, g0) + lead_dot(hid, g1)).astype(BF16)

    with jax.named_scope("up"):
        for t in range(2):
            for q in range(2):
                if t == 0:
                    local[2 * q].wait()
                    local[2 * q + 1].wait()
                up(t, q)
        xt[...] = xs[...].reshape(TOKENS, DL).T
        xt_copy = local_copy(xt, xt_out, 9)
    with jax.named_scope("ring"):
        for s in range(1, 4):
            for t in range(2):
                for q in range(2):
                    for d in range(2):
                        if s > (0 if d == long_way(q, t) else 1):
                            ring(t, q, d, s)
    for t in range(2):
        with jax.named_scope("hidden%d" % t):
            hidden(t)
    for t in range(2):
        with jax.named_scope("relay%d" % t):
            for d in range(2):
                relay(0, t, d)
    for c in local[4:]:
        c.wait()
    own_tgt.wait()
    for t in range(2):
        with jax.named_scope("out%d" % t):
            out(t)
        with jax.named_scope("outs%d" % t):
            out_send(t)
    for t in range(2):
        with jax.named_scope("grads%d" % t):
            grads(t)
    for t in range(2):
        with jax.named_scope("gradson%d" % t):
            grads_on(t)
        with jax.named_scope("back%d" % t):
            back(t)
    with jax.named_scope("down"):
        down(0)
        down(256)
        hd_copy = local_copy(hd, hd_out, 10)
    for t in range(2):
        with jax.named_scope("fold%d" % t):
            for d in range(2):
                fold(t, d)
    for t in range(2):
        with jax.named_scope("inner%d" % t):
            inner(t)
    for t in range(2):
        with jax.named_scope("relayb%d" % t):
            for d in range(2):
                relay(1, t, d)
    for t in range(2):
        with jax.named_scope("gathered%d" % t):
            gathered(1, t)
    with jax.named_scope("tail"):
        ag_copy = local_copy(ag.at[1], ag_out, 11)
        left(xs.at[:, pl.ds(0, 56), :], xsem.at[0])
        left(xs.at[:, pl.ds(0, 64), :], xsem.at[2])
        left(sbuf, rss)
        left(pbuf, pss)
        left(ag.at[:, :, :, pl.ds(0, 120), :], ags)
        left(osend, oss.at[0])
        left(oown.at[:, pl.ds(0, 7)], oss.at[1])
        left(gs.at[:, :, pl.ds(0, 56), :], gss.at[0])
        left(gs.at[:, :, pl.ds(0, 64), :], gss.at[1])
        xt_copy.wait()
        hd_copy.wait()
        ag_copy.wait()


def weights_kernel(xt, ag, hd, gate_out, up_out, down_out, buf, sem):
    rows = DL // 4
    down = pltpu.make_async_copy(hd, down_out, sem.at[8])
    down.start()
    copies = []
    for v, out in enumerate((gate_out, up_out)):
        for i in range(4):
            part = pl.ds(i * rows, rows)
            buf[v, part, :] = jnp.dot(xt[part, :], ag[v], preferred_element_type=F32).astype(BF16)
            copy = pltpu.make_async_copy(buf.at[v, part, :], out.at[part, :], sem.at[4 * v + i])
            copy.start()
            copies.append(copy)
    down.wait()
    for copy in copies:
        copy.wait()


def body(*args):
    hbm = pl.BlockSpec(memory_space=pltpu.HBM)
    vmem = pl.BlockSpec(memory_space=pltpu.VMEM)
    dma = pltpu.SemaphoreType.DMA
    args = [pltpu.with_memory_space_constraint(a, pltpu.HBM) for a in args]
    xt, ag, hd = pl.pallas_call(
        kernel,
        out_shape=(
            jax.ShapeDtypeStruct((DL, TOKENS), BF16),
            jax.ShapeDtypeStruct((2, 2, 128, FL), BF16),
            jax.ShapeDtypeStruct((FL, DL), BF16),
        ),
        in_specs=[hbm] * 8,
        out_specs=(pl.BlockSpec(memory_space=pl.ANY),) * 3,
        scratch_shapes=[
            pltpu.VMEM((2, 128, DL), BF16),
            pltpu.VMEM((DL, TOKENS), BF16),
            pltpu.VMEM((FL, DL), BF16),
            pltpu.VMEM((TOKENS // NG, DL), BF16),
            pltpu.VMEM((4, DL, FL), BF16),
            pltpu.VMEM((2, FL, DL), BF16),
            pltpu.VMEM((2, 3, 16, 2, 8, FL), F32),
            pltpu.VMEM((6, 7, 2, 2, 8, FL), BF16),
            pltpu.VMEM((6, 2, 3, 2, 2, 8, FL), BF16),
            pltpu.VMEM((6, 2, 8, FL), BF16),
            pltpu.VMEM((6, 9, 2, 8, FL), BF16),
            pltpu.VMEM((2, 4, 8, FL), F32),
            pltpu.VMEM((2, 2, 2, 128, FL), BF16),
            pltpu.VMEM((2, 2, 8, 2, 8, DL), F32),
            pltpu.VMEM((2, 8, 2, 8, DL), BF16),
            pltpu.VMEM((2, 8, 2, 8, DL), BF16),
            pltpu.VMEM((2, 8, 2, 8, DL), BF16),
            pltpu.VMEM((2, 8, 2, 8, DL), BF16),
            pltpu.VMEM((2, 2, 128, DL), BF16),
            dma((12,)),
            dma((4,)),
            dma, dma,
            dma((6, 2, 3)),
            dma((6,)),
            dma,
            dma((2, 2, 3)),
            dma((2,)), dma((4,)),
            dma((2,)), dma((4,)),
        ],
        compiler_params=pltpu.CompilerParams(
            collective_id=0, has_side_effects=True, vmem_limit_bytes=40 * 1024 * 1024
        ),
    )(*args)
    return pl.pallas_call(
        weights_kernel,
        out_shape=(
            jax.ShapeDtypeStruct((DL, FL), BF16),
            jax.ShapeDtypeStruct((DL, FL), BF16),
            jax.ShapeDtypeStruct((FL, DL), BF16),
        ),
        in_specs=[vmem] * 3,
        out_specs=(hbm,) * 3,
        scratch_shapes=[pltpu.VMEM((2, DL, FL), BF16), dma((9,))],
        compiler_params=pltpu.CompilerParams(vmem_limit_bytes=16 * 1024 * 1024),
    )(xt, ag.reshape(2, TOKENS, FL), hd)


def solution(mesh):
    in_specs = (
        P("gy", "gx"),
        P("gy", "gx"),
        P("gx", "gy"),
        P("gx", "gy"),
        P("gy", "gx"),
        P("gx", "gy"),
        P("gx", "gy"),
        P("gy", "gx"),
    )
    out_specs = (P("gx", "gy"), P("gx", "gy"), P("gy", "gx"))
    return jax.shard_map(body, mesh=mesh, in_specs=in_specs, out_specs=out_specs, check_vma=False)
```

```python
import functools
import math

import jax
import jax.numpy as jnp
from jax import lax
from jax.experimental import pallas as pl
from jax.experimental.pallas import tpu as pltpu
from jax.sharding import PartitionSpec as P

MESH = pl.DeviceIdType.MESH
TOKENS = 256
DL = 512
FL = 896
NZ = 8
NG = 16
F32 = jnp.float32
BF16 = jnp.bfloat16


def silu_parts(gate):
    sig = jax.nn.sigmoid(gate)
    first = sig * (1.0 + gate * (1.0 - sig))
    second = sig * (1.0 - sig) * (2.0 + gate * (1.0 - 2.0 * sig))
    return (gate * sig, first, second)


def lead_dot(left, right):
    return lax.dot_general(left, right, (((0,), (0,)), ((), ())), preferred_element_type=F32)


def tail_dot(left, right):
    return lax.dot_general(left, right, (((1,), (1,)), ((), ())), preferred_element_type=F32)


TINY = 1e-36


def encode2(v):
    return (v * jnp.abs(v)).astype(BF16)


def decode2(c):
    v = c.astype(F32)
    return v * lax.rsqrt(jnp.maximum(jnp.abs(v), TINY))


def encode4(v):
    return (v * jnp.abs(v) * (v * v)).astype(BF16)


def decode4(c):
    v = c.astype(F32)
    w = lax.rsqrt(jnp.maximum(jnp.abs(v), TINY))
    return v * w * (w * lax.rsqrt(w))


ORDER = (
    ("up", 0, 1), ("cross0", 0), ("up", 0, 0), ("start", 0), ("up", 1, 1), ("cross0", 1), ("cross1", 0), ("up", 1, 0), ("start", 1), ("cross1", 1),
    ("half", 0, 0, 0), ("half", 0, 1, 1), ("full", 0, 0, 1), ("half", 1, 0, 0), ("half", 1, 1, 1), ("full", 1, 0, 1), ("flat", 0), ("flat", 1),
    ("half", 0, 0, 1), ("full", 0, 0, 2), ("full", 0, 1, 2), ("half", 1, 0, 1), ("full", 1, 0, 2), ("full", 1, 1, 2),
    ("half", 0, 0, 2), ("half", 0, 1, 2), ("full", 0, 0, 3), ("full", 0, 1, 3), ("half", 1, 0, 2), ("half", 1, 1, 2), ("full", 1, 0, 3), ("full", 1, 1, 3),
    ("half", 0, 0, 3), ("half", 0, 1, 3), ("half", 1, 0, 3), ("half", 1, 1, 3),
    ("hidden", 0), ("hidden", 1), ("pass", 0), ("pass", 1), ("out", 0), ("outs", 0), ("out", 1), ("outs", 1),
    ("grads", 0), ("grads", 1), ("on", 0), ("back", 0), ("on", 1), ("back", 1), ("down", 0), ("down", 256),
    ("fold", 0), ("fold", 1), ("inner", 0), ("inner", 1), ("pass1", 0), ("pass1", 1),
)


def kernel(
    tok, tgt, wg, wu, wd, tg, tu, td,
    xt_out, ag_out, hd_out,
    xs, xt, hd, tgv, wup, wdn, part, sbuf, rbuf, pbuf, fin, ysb, yrb, hsb, hrb, act, ag, osum, osend, ocore, oown, orecv, gs,
    lsem, xsem, rss, pss, rsr, fsr, yss, ysr, hss, hsr, ags, agr, oss, osr, gss, gsr,
):
    scale = 1.0 / math.sqrt(TOKENS)
    g = lax.axis_index("gx")
    h = lax.axis_index("gy")
    core = lax.rem(h, 2)
    mine = lax.div(h, 2)
    mate = h + 1 - 2 * core
    yh = lax.div(g, NZ)
    z = lax.rem(g, NZ)
    own8 = pl.ds(pl.multiple_of(64 * core + 8 * mine, 8), 8)
    core64 = pl.ds(pl.multiple_of(64 * core, 64), 64)
    zown = pl.ds(pl.multiple_of(16 * z + 8 * yh, 8), 8)

    def zat(k):
        return lax.rem(z + k + NZ, NZ)

    def column(k, other=False):
        y = 1 - yh if other else yh
        return {"gx": y * NZ + zat(k)}

    def at_gy(i):
        return {"gy": i}

    def way(d, k):
        return k if d == 0 else -k

    def send(src, dst, ssem, rsem, where):
        pltpu.make_async_remote_copy(
            src_ref=src, dst_ref=dst, send_sem=ssem, recv_sem=rsem, device_id=where, device_id_type=MESH
        ).start()

    def arrived(ref, sem):
        pltpu.make_async_remote_copy(
            src_ref=ref, dst_ref=ref, send_sem=sem, recv_sem=sem, device_id=at_gy(mate), device_id_type=MESH
        ).wait_recv()

    def left(ref, sem):
        pltpu.make_async_remote_copy(
            src_ref=ref, dst_ref=ref, send_sem=sem, recv_sem=sem, device_id=at_gy(mate), device_id_type=MESH
        ).wait_send()

    def local_copy(src, dst, i):
        copy = pltpu.make_async_copy(src, dst, lsem.at[i])
        copy.start()
        return copy

    own_tok = [local_copy(tok.at[pl.ds(8 * t, 8), :], xs.at[t, own8, :], t) for t in range(2)]
    local = [local_copy(w, wup.at[i], 2 + i) for i, w in enumerate((wg, wu, tg, tu))]
    local += [local_copy(w, wdn.at[i], 6 + i) for i, w in enumerate((wd, td))]
    own_tgt = local_copy(tgt, tgv, 8)

    with jax.named_scope("barrier"):
        barrier = pltpu.get_barrier_semaphore()
        near = [column(k, o) for k in (1, -1, 2, -2) for o in (False, True)] + [column(0, True)]
        near += [at_gy(lax.rem(h + 2 * k, NG)) for k in range(1, 8)] + [at_gy(mate)]
        for where in near:
            pl.semaphore_signal(barrier, inc=1, device_id=where, device_id_type=MESH)
        pl.semaphore_wait(barrier, len(near))

    far = (4, 5, 3, 6, 2, 7, 1)

    def spread(block, ssem, rsem):
        for k in far:
            send(block, block, ssem, rsem, at_gy(lax.rem(h + 2 * k, NG)))

    def hand_on(seven, eight, rsem, dsem, drsem):
        arrived(seven, rsem)
        send(eight, eight, dsem, drsem, at_gy(mate))

    with jax.named_scope("tokens"):
        for c in own_tok:
            c.wait()
        spread(xs.at[:, own8, :], xsem.at[0], xsem.at[1])
        hand_on(xs.at[:, pl.ds(0, 56), :], xs.at[:, core64, :], xsem.at[1], xsem.at[2], xsem.at[3])
        arrived(xs.at[:, pl.ds(0, 64), :], xsem.at[3])

    slots = {}

    def slot_of(tq):
        slots[tq] = slots.get(tq, -1) + 1
        return slots[tq]

    def enc(q, v):
        return encode4(v) if q < 2 else encode2(v)

    def dec(q, v):
        return decode4(v) if q < 2 else decode2(v)

    def long_way(q, t):
        return (q + t) % 2

    def chunk(t, q, d, k):
        return part[t, q, zat(way(d, k))]

    def send_whole(t, q, val, d, hops, slot):
        tq = 2 * t + q // 2
        i = slot_of(tq)
        sbuf[tq, i] = enc(q, val)
        send(sbuf.at[tq, i], rbuf.at[tq, d, slot], rss, rsr.at[tq, d, slot], column(way(d, hops)))

    def send_last(t, q, val, d, hops, slot):
        tq = 2 * t + q // 2
        i = slot_of(tq)
        sbuf[tq, i] = enc(q, val)
        for other in (True, False):
            y = 1 - yh if other else yh
            dst = fin.at[tq, slot + d + (2 if other else 0)]
            send(sbuf.at[tq, i, y], dst, rss, fsr.at[tq], column(way(d, hops), other))

    def send_pair(t, q):
        tq = 2 * t + q // 2
        pbuf[tq] = enc(q, part[t, q, z, 1 - yh])
        send(pbuf.at[tq], fin.at[tq, 4], pss, fsr.at[tq], column(0, True))

    def taken(t, q, d, slot):
        tq = 2 * t + q // 2
        arrived(rbuf.at[tq, d, slot], rsr.at[tq, d, slot])
        return dec(q, rbuf[tq, d, slot])

    def total(t, q, n):
        tq = 2 * t + q // 2
        arrived(fin.at[tq, pl.ds(0, n)], fsr.at[tq])
        val = part[t, q, z, yh]
        for i in range(n):
            val = val + dec(q, fin[tq, i])
        return val

    def up(t, q):
        for u in range(2):
            for n in range(0, FL, 256):
                m = min(256, FL - n)
                val = jnp.dot(xs[t], wup[2 * q + u, :, n : n + m], preferred_element_type=F32)
                part[t, q, :, :, u, :, n : n + m] = val.reshape(8, 2, 8, m)

    def ring_start(t):
        d = long_way(0, t)
        send_whole(t, 0, chunk(t, 0, d, 4), d, 1, 0)
        send_whole(t, 0, chunk(t, 0, 1 - d, 3), 1 - d, 1, 1)
        send_pair(t, 0)

    def ring(t, q, d, s):
        val = chunk(t, q, d, 4 - s) + taken(t, q, d, s - 1)
        if s < 3:
            send_whole(t, q, val, d, 1, s)
        else:
            send_last(t, q, val, d, 1, 0)

    def cross(t, ks):
        d = long_way(1, t)
        for k in ks:
            i = way(d, k) % NZ
            ysb[t, i] = enc(0, part[t, 1, zat(i), 1 - yh])
            send(ysb.at[t, i], yrb.at[t, i], yss, ysr.at[t, i], column(0, True))

    def crossed(t, k):
        i = k % NZ
        arrived(yrb.at[t, i], ysr.at[t, i])
        return part[t, 1, zat(i), yh] + dec(0, yrb[t, i])

    def half_ring(t, d, s):
        val = crossed(t, way(d, 4 - s))
        first = 0 if d == long_way(1, t) else 1
        if s > first:
            arrived(hrb.at[t, d, s - 1], hsr.at[t, d, s - 1])
            val = val + dec(0, hrb[t, d, s - 1])
        i = slot_of(10 + t)
        hsb[t, i] = enc(0, val)
        send(hsb.at[t, i], hrb.at[t, d, s], hss, hsr.at[t, d, s], column(way(d, 1)))

    def half_total(t):
        val = crossed(t, 0)
        for d in range(2):
            arrived(hrb.at[t, d, 3], hsr.at[t, d, 3])
            val = val + dec(0, hrb[t, d, 3])
        return val

    def gather(v, t):
        own = ag.at[v, :, t, zown, :]
        for d in range(2):
            for other in (True, False):
                send(own, own, ags, agr.at[t, v, d], column(way(d, 2), other))
        for d in range(2):
            for other in (True, False):
                send(own, own, ags, agr.at[t, v, 2], column(way(d, 1), other))
        send(own, own, ags, agr.at[t, v, 2], column(0, True))

    def relay(v, t, d):
        arrived(ag.at[v, :, t, pl.ds(0, 16), :], agr.at[t, v, d])
        rows = ag.at[v, :, t, pl.ds(pl.multiple_of(16 * zat(way(d, -2)), 16), 16), :]
        if d == long_way(v, t):
            send(rows, rows, ags, agr.at[t, v, 2], column(way(d, 2)))
        send(rows, rows, ags, agr.at[t, v, 2], column(way(d, 1)))

    def gathered(v, t):
        arrived(ag.at[v, :, t, pl.ds(0, 88), :], agr.at[t, v, 2])

    def hidden(t):
        val = total(t, 0, 5)
        gate, upper = val[0], val[1]
        val = half_total(t)
        gate_dot, upper_dot = val[0], val[1]
        silu_val, first, second = silu_parts(gate)
        ag[0, 0, t, zown, :] = (silu_val * upper).astype(BF16)
        ag[0, 1, t, zown, :] = (first * gate_dot * upper + silu_val * upper_dot).astype(BF16)
        gather(0, t)
        for i, a in enumerate((gate, upper, gate_dot, upper_dot)):
            act[t, i] = a

    def out(t):
        gathered(0, t)
        for n in range(0, DL, 256):
            cols = slice(n, n + 256)
            val = jnp.dot(ag[0, 0, t], wdn[0, :, cols], preferred_element_type=F32)
            osum[t, :, :, 0, :, cols] = val.reshape(2, 8, 8, 256)
            val = jnp.dot(ag[0, 1, t], wdn[0, :, cols], preferred_element_type=F32)
            val = val + jnp.dot(ag[0, 0, t], wdn[1, :, cols], preferred_element_type=F32)
            osum[t, :, :, 1, :, cols] = val.reshape(2, 8, 8, 256)
        osend[t] = encode2(osum[t, 1 - core])
        send(osend.at[t], ocore.at[t], oss.at[0], osr.at[t], at_gy(mate))

    def out_send(t):
        arrived(ocore.at[t], osr.at[t])
        val = osum[t, core] + decode2(ocore[t])
        osum[t, core] = val
        oown[t] = encode2(val)
        for k in far:
            dst = lax.rem(mine + k, 8)
            send(oown.at[t, dst], orecv.at[t, k], oss.at[1], osr.at[2 + t], at_gy(2 * dst + core))

    def grads(t):
        arrived(orecv.at[t, pl.ds(1, 7)], osr.at[2 + t])
        val = osum[t, core, mine]
        for k in range(1, 8):
            val = val + decode2(orecv[t, k])
        target = tgv[8 * t : 8 * t + 8, :].astype(F32)
        gs[t, 0, own8, :] = ((val[0] - target) * scale).astype(BF16)
        gs[t, 1, own8, :] = (val[1] * scale).astype(BF16)
        spread(gs.at[t, :, own8, :], gss.at[0], gsr.at[t])

    def grads_on(t):
        hand_on(gs.at[t, :, pl.ds(0, 56), :], gs.at[t, :, core64, :], gsr.at[t], gss.at[1], gsr.at[2 + t])

    def back(t):
        arrived(gs.at[t, :, pl.ds(0, 64), :], gsr.at[2 + t])
        for n in range(0, FL, 256):
            m = min(256, FL - n)
            val = tail_dot(gs[t, 0], wdn[0, n : n + m, :])
            part[t, 2, :, :, 0, :, n : n + m] = val.reshape(8, 2, 8, m)
            val = tail_dot(gs[t, 1], wdn[0, n : n + m, :]) + tail_dot(gs[t, 0], wdn[1, n : n + m, :])
            part[t, 2, :, :, 1, :, n : n + m] = val.reshape(8, 2, 8, m)
        for d in range(2):
            send_whole(t, 2, chunk(t, 2, d, 3), d, 1, 0)
        d = long_way(2, t)
        send_whole(t, 2, chunk(t, 2, d, 4), d, 2, 1)
        for d in range(2):
            send_last(t, 2, chunk(t, 2, d, 1), d, 1, 0)
        send_pair(t, 2)

    def fold(t, d):
        val = chunk(t, 2, d, 2) + taken(t, 2, d, 0)
        if d == long_way(2, t):
            val = val + taken(t, 2, d, 1)
        send_last(t, 2, val, d, 2, 5)

    def inner(t):
        val = total(t, 2, 9)
        back_val, back_dot = val[0], val[1]
        gate, upper, gate_dot, upper_dot = act[t, 0], act[t, 1], act[t, 2], act[t, 3]
        silu_val, first, second = silu_parts(gate)
        ag[1, 0, t, zown, :] = (
            back_dot * upper * first + back_val * upper_dot * first + back_val * upper * second * gate_dot
        ).astype(BF16)
        ag[1, 1, t, zown, :] = (back_dot * silu_val + back_val * first * gate_dot).astype(BF16)
        gather(1, t)

    def down(n):
        g0 = gs[:, 0, :, n : n + 256].reshape(TOKENS, 256)
        g1 = gs[:, 1, :, n : n + 256].reshape(TOKENS, 256)
        hid = ag[0, 0].reshape(TOKENS, FL)
        hid_dot = ag[0, 1].reshape(TOKENS, FL)
        hd[:, n : n + 256] = (lead_dot(hid_dot, g0) + lead_dot(hid, g1)).astype(BF16)

    def flat(t):
        xt[:, 128 * t : 128 * t + 128] = xs[t].T

    def both(f, *a):
        for d in range(2):
            f(*a, d)

    def up_waited(t, q):
        if t == 0:
            local[2 * q].wait()
            local[2 * q + 1].wait()
        up(t, q)

    def out_waited(t):
        if t == 0:
            for c in local[4:]:
                c.wait()
            own_tgt.wait()
        out(t)

    def half_way(t, short, s):
        half_ring(t, (long_way(1, t) + short) % 2, s)

    def full_way(t, short, s):
        ring(t, 0, (long_way(0, t) + short) % 2, s)

    steps = {
        "up": up_waited,
        "cross0": lambda t: cross(t, (4, -3, 3)),
        "cross1": lambda t: cross(t, (2, -2, 1, -1, 0)),
        "start": ring_start,
        "half": half_way,
        "full": full_way,
        "hidden": hidden,
        "pass": lambda t: both(relay, 0, t),
        "out": out_waited,
        "outs": out_send,
        "grads": grads,
        "on": grads_on,
        "back": back,
        "fold": lambda t: both(fold, t),
        "inner": inner,
        "pass1": lambda t: both(relay, 1, t),
        "down": down,
        "flat": flat,
    }
    for name, *a in ORDER:
        with jax.named_scope(name + "_".join(str(i) for i in a)):
            steps[name](*a)
    xt_copy = local_copy(xt, xt_out, 9)
    hd_copy = local_copy(hd, hd_out, 10)
    for t in range(2):
        with jax.named_scope("gathered%d" % t):
            gathered(1, t)
    with jax.named_scope("tail"):
        ag_copy = local_copy(ag.at[1], ag_out, 11)
        left(xs.at[:, pl.ds(0, 56), :], xsem.at[0])
        left(xs.at[:, pl.ds(0, 64), :], xsem.at[2])
        left(sbuf, rss)
        left(pbuf, pss)
        left(ysb, yss)
        left(hsb, hss)
        left(ag.at[:, :, :, pl.ds(0, 120), :], ags)
        left(osend, oss.at[0])
        left(oown.at[:, pl.ds(0, 7)], oss.at[1])
        left(gs.at[:, :, pl.ds(0, 56), :], gss.at[0])
        left(gs.at[:, :, pl.ds(0, 64), :], gss.at[1])
        xt_copy.wait()
        hd_copy.wait()
        ag_copy.wait()


def weights_kernel(xt, ag, hd, gate_out, up_out, down_out, buf, sem):
    rows = DL // 4
    down = pltpu.make_async_copy(hd, down_out, sem.at[8])
    down.start()
    copies = []
    for v, out in enumerate((gate_out, up_out)):
        for i in range(4):
            part = pl.ds(i * rows, rows)
            buf[v, part, :] = jnp.dot(xt[part, :], ag[v], preferred_element_type=F32).astype(BF16)
            copy = pltpu.make_async_copy(buf.at[v, part, :], out.at[part, :], sem.at[4 * v + i])
            copy.start()
            copies.append(copy)
    down.wait()
    for copy in copies:
        copy.wait()


def body(*args):
    hbm = pl.BlockSpec(memory_space=pltpu.HBM)
    vmem = pl.BlockSpec(memory_space=pltpu.VMEM)
    dma = pltpu.SemaphoreType.DMA
    args = [pltpu.with_memory_space_constraint(a, pltpu.HBM) for a in args]
    xt, ag, hd = pl.pallas_call(
        kernel,
        out_shape=(
            jax.ShapeDtypeStruct((DL, TOKENS), BF16),
            jax.ShapeDtypeStruct((2, 2, 128, FL), BF16),
            jax.ShapeDtypeStruct((FL, DL), BF16),
        ),
        in_specs=[hbm] * 8,
        out_specs=(pl.BlockSpec(memory_space=pl.ANY),) * 3,
        scratch_shapes=[
            pltpu.VMEM((2, 128, DL), BF16),
            pltpu.VMEM((DL, TOKENS), BF16),
            pltpu.VMEM((FL, DL), BF16),
            pltpu.VMEM((TOKENS // NG, DL), BF16),
            pltpu.VMEM((4, DL, FL), BF16),
            pltpu.VMEM((2, FL, DL), BF16),
            pltpu.VMEM((2, 3, 8, 2, 2, 8, FL), F32),
            pltpu.VMEM((4, 7, 2, 2, 8, FL), BF16),
            pltpu.VMEM((4, 2, 3, 2, 2, 8, FL), BF16),
            pltpu.VMEM((4, 2, 8, FL), BF16),
            pltpu.VMEM((4, 9, 2, 8, FL), BF16),
            pltpu.VMEM((2, 8, 2, 8, FL), BF16),
            pltpu.VMEM((2, 8, 2, 8, FL), BF16),
            pltpu.VMEM((2, 7, 2, 8, FL), BF16),
            pltpu.VMEM((2, 2, 4, 2, 8, FL), BF16),
            pltpu.VMEM((2, 4, 8, FL), F32),
            pltpu.VMEM((2, 2, 2, 128, FL), BF16),
            pltpu.VMEM((2, 2, 8, 2, 8, DL), F32),
            pltpu.VMEM((2, 8, 2, 8, DL), BF16),
            pltpu.VMEM((2, 8, 2, 8, DL), BF16),
            pltpu.VMEM((2, 8, 2, 8, DL), BF16),
            pltpu.VMEM((2, 8, 2, 8, DL), BF16),
            pltpu.VMEM((2, 2, 128, DL), BF16),
            dma((12,)),
            dma((4,)),
            dma, dma,
            dma((4, 2, 3)),
            dma((4,)),
            dma, dma((2, 8)),
            dma, dma((2, 2, 4)),
            dma,
            dma((2, 2, 3)),
            dma((2,)), dma((4,)),
            dma((2,)), dma((4,)),
        ],
        compiler_params=pltpu.CompilerParams(
            collective_id=0, has_side_effects=True, vmem_limit_bytes=40 * 1024 * 1024
        ),
    )(*args)
    return pl.pallas_call(
        weights_kernel,
        out_shape=(
            jax.ShapeDtypeStruct((DL, FL), BF16),
            jax.ShapeDtypeStruct((DL, FL), BF16),
            jax.ShapeDtypeStruct((FL, DL), BF16),
        ),
        in_specs=[vmem] * 3,
        out_specs=(hbm,) * 3,
        scratch_shapes=[pltpu.VMEM((2, DL, FL), BF16), dma((9,))],
        compiler_params=pltpu.CompilerParams(vmem_limit_bytes=16 * 1024 * 1024),
    )(xt, ag.reshape(2, TOKENS, FL), hd)


def solution(mesh):
    in_specs = (
        P("gy", "gx"),
        P("gy", "gx"),
        P("gx", "gy"),
        P("gx", "gy"),
        P("gy", "gx"),
        P("gx", "gy"),
        P("gx", "gy"),
        P("gy", "gx"),
    )
    out_specs = (P("gx", "gy"), P("gx", "gy"), P("gy", "gx"))
    return jax.shard_map(body, mesh=mesh, in_specs=in_specs, out_specs=out_specs, check_vma=False)
```

```python
import functools
import math

import jax
import jax.numpy as jnp
from jax import lax
from jax.experimental import pallas as pl
from jax.experimental.pallas import tpu as pltpu
from jax.sharding import PartitionSpec as P

MESH = pl.DeviceIdType.MESH
TOKENS = 256
DL = 512
FL = 896
NZ = 8
NG = 16
F32 = jnp.float32
BF16 = jnp.bfloat16


def silu_parts(gate):
    sig = jax.nn.sigmoid(gate)
    first = sig * (1.0 + gate * (1.0 - sig))
    second = sig * (1.0 - sig) * (2.0 + gate * (1.0 - 2.0 * sig))
    return (gate * sig, first, second)


def lead_dot(left, right):
    return lax.dot_general(left, right, (((0,), (0,)), ((), ())), preferred_element_type=F32)


def tail_dot(left, right):
    return lax.dot_general(left, right, (((1,), (1,)), ((), ())), preferred_element_type=F32)


TINY = 1e-36


def encode2(v):
    return (v * jnp.abs(v)).astype(BF16)


def decode2(c):
    v = c.astype(F32)
    return v * lax.rsqrt(jnp.maximum(jnp.abs(v), TINY))


def encode4(v):
    return (v * jnp.abs(v) * (v * v)).astype(BF16)


def decode4(c):
    v = c.astype(F32)
    w = lax.rsqrt(jnp.maximum(jnp.abs(v), TINY))
    return v * w * (w * lax.rsqrt(w))


ORDER = (
    ("up", 0, 1), ("cross0", 0), ("up", 0, 0), ("start", 0), ("up", 1, 1), ("cross0", 1), ("cross1", 0), ("up", 1, 0), ("start", 1), ("cross1", 1),
    ("full", 0, 0, 1), ("half", 0, 0, 0), ("half", 0, 1, 1), ("full", 1, 0, 1), ("half", 1, 0, 0), ("half", 1, 1, 1), ("full", 0, 0, 2),
    ("full", 0, 1, 2), ("half", 0, 0, 1), ("full", 1, 0, 2), ("full", 1, 1, 2), ("half", 1, 0, 1), ("full", 0, 0, 3), ("full", 0, 1, 3),
    ("half", 0, 0, 2), ("half", 0, 1, 2), ("full", 1, 0, 3), ("full", 1, 1, 3), ("half", 1, 0, 2), ("half", 1, 1, 2), ("flat", 0), ("flat", 1),
    ("hidden", 0), ("half", 0, 0, 3), ("half", 0, 1, 3), ("hidden", 1), ("half", 1, 0, 3), ("half", 1, 1, 3), ("hiddent", 0), ("hiddent", 1),
    ("pass", 0), ("pass", 1), ("passt", 0), ("passt", 1), ("out", 0, 0), ("out", 1, 0), ("outs", 0, 0), ("outs", 1, 0), ("out", 0, 1), ("out", 1, 1),
    ("outs", 0, 1), ("outs", 1, 1), ("grads", 0, 0), ("grads", 1, 0), ("grads", 0, 1), ("grads", 1, 1), ("back", 0, 0), ("back", 1, 0),
    ("back", 0, 1), ("back", 1, 1), ("down", 0), ("down", 256), ("fold", 0, 0), ("fold", 1, 0), ("fold", 0, 1), ("fold", 1, 1), ("inner", 0),
    ("inner", 1), ("pass1", 0), ("pass1", 1),
)


def kernel(
    tok, tgt, wg, wu, wd, tg, tu, td,
    xt_out, ag_out, hd_out,
    xs, xt, hd, tgv, wup, wdn, part, sbuf, rbuf, pbuf, fin, ysb, yrb, hsb, hrb, bsb, brb, bpb, bfin, act, ag, osum, osend, ocore, oown, orecv, gs,
    lsem, xsem, rss, pss, rsr, fsr, yss, ysr, hss, hsr, bsb_sem, brb_sem, bpb_sem, bfin_sem, ags, agr, oss, osr, gss, gsr,
):
    scale = 1.0 / math.sqrt(TOKENS)
    g = lax.axis_index("gx")
    h = lax.axis_index("gy")
    core = lax.rem(h, 2)
    mine = lax.div(h, 2)
    mate = h + 1 - 2 * core
    yh = lax.div(g, NZ)
    z = lax.rem(g, NZ)
    own8 = pl.ds(pl.multiple_of(64 * core + 8 * mine, 8), 8)
    core64 = pl.ds(pl.multiple_of(64 * core, 64), 64)
    zown = pl.ds(pl.multiple_of(16 * z + 8 * yh, 8), 8)

    def zat(k):
        return lax.rem(z + k + NZ, NZ)

    def column(k, other=False):
        y = 1 - yh if other else yh
        return {"gx": y * NZ + zat(k)}

    def at_gy(i):
        return {"gy": i}

    def way(d, k):
        return k if d == 0 else -k

    def send(src, dst, ssem, rsem, where):
        pltpu.make_async_remote_copy(
            src_ref=src, dst_ref=dst, send_sem=ssem, recv_sem=rsem, device_id=where, device_id_type=MESH
        ).start()

    def arrived(ref, sem):
        pltpu.make_async_remote_copy(
            src_ref=ref, dst_ref=ref, send_sem=sem, recv_sem=sem, device_id=at_gy(mate), device_id_type=MESH
        ).wait_recv()

    def left(ref, sem):
        pltpu.make_async_remote_copy(
            src_ref=ref, dst_ref=ref, send_sem=sem, recv_sem=sem, device_id=at_gy(mate), device_id_type=MESH
        ).wait_send()

    def local_copy(src, dst, i):
        copy = pltpu.make_async_copy(src, dst, lsem.at[i])
        copy.start()
        return copy

    own_tok = [local_copy(tok.at[pl.ds(8 * t, 8), :], xs.at[t, own8, :], t) for t in range(2)]
    local = [local_copy(w, wup.at[i], 2 + i) for i, w in enumerate((wg, wu, tg, tu))]
    local += [local_copy(w, wdn.at[i], 6 + i) for i, w in enumerate((wd, td))]
    own_tgt = local_copy(tgt, tgv, 8)

    with jax.named_scope("barrier"):
        barrier = pltpu.get_barrier_semaphore()
        near = [column(k, o) for k in (1, -1, 2, -2) for o in (False, True)] + [column(0, True)]
        near += [at_gy(lax.rem(h + k, NG)) for k in range(1, NG)]
        for where in near:
            pl.semaphore_signal(barrier, inc=1, device_id=where, device_id_type=MESH)
        pl.semaphore_wait(barrier, len(near))

    far = (4, 5, 3, 6, 2, 7, 1)
    all_far = (8, 10, 6, 9, 7, 11, 5, 12, 4, 14, 2, 13, 3, 15, 1)

    with jax.named_scope("tokens"):
        for c in own_tok:
            c.wait()
        for k in all_far:
            send(xs.at[:, own8, :], xs.at[:, own8, :], xsem.at[0], xsem.at[1], at_gy(lax.rem(h + k, NG)))
        arrived(xs.at[:, pl.ds(0, 120), :], xsem.at[1])

    slots = {}

    def slot_of(tq):
        slots[tq] = slots.get(tq, -1) + 1
        return slots[tq]

    def enc(q, v):
        return encode4(v) if q < 2 else encode2(v)

    def dec(q, v):
        return decode4(v) if q < 2 else decode2(v)

    def long_way(q, t):
        return (q + t) % 2

    def chunk(t, q, d, k):
        return part[t, q, zat(way(d, k))]

    def send_whole(t, q, val, d, hops, slot):
        tq = t
        i = slot_of(tq)
        sbuf[tq, i] = enc(q, val)
        send(sbuf.at[tq, i], rbuf.at[tq, d, slot], rss, rsr.at[tq, d, slot], column(way(d, hops)))

    def send_last(t, q, val, d, hops, slot):
        tq = t
        i = slot_of(tq)
        sbuf[tq, i] = enc(q, val)
        for other in (True, False):
            y = 1 - yh if other else yh
            dst = fin.at[tq, slot + d + (2 if other else 0)]
            send(sbuf.at[tq, i, y], dst, rss, fsr.at[tq], column(way(d, hops), other))

    def send_pair(t, q):
        tq = t
        pbuf[tq] = enc(q, part[t, q, z, 1 - yh])
        send(pbuf.at[tq], fin.at[tq, 4], pss, fsr.at[tq], column(0, True))

    def taken(t, q, d, slot):
        tq = t
        arrived(rbuf.at[tq, d, slot], rsr.at[tq, d, slot])
        return dec(q, rbuf[tq, d, slot])

    def total(t, q, n):
        tq = t
        arrived(fin.at[tq, pl.ds(0, n)], fsr.at[tq])
        val = part[t, q, z, yh]
        for i in range(n):
            val = val + dec(q, fin[tq, i])
        return val

    def up(t, q):
        for u in range(2):
            for n in range(0, FL, 256):
                m = min(256, FL - n)
                val = jnp.dot(xs[t], wup[2 * q + u, :, n : n + m], preferred_element_type=F32)
                part[t, q, :, :, u, :, n : n + m] = val.reshape(8, 2, 8, m)

    def ring_start(t):
        d = long_way(0, t)
        send_whole(t, 0, chunk(t, 0, d, 4), d, 1, 0)
        send_whole(t, 0, chunk(t, 0, 1 - d, 3), 1 - d, 1, 1)
        send_pair(t, 0)

    def ring(t, q, d, s):
        val = chunk(t, q, d, 4 - s) + taken(t, q, d, s - 1)
        if s < 3:
            send_whole(t, q, val, d, 1, s)
        else:
            send_last(t, q, val, d, 1, 0)

    def cross(t, ks):
        d = long_way(1, t)
        for k in ks:
            i = way(d, k) % NZ
            ysb[t, i] = enc(0, part[t, 1, zat(i), 1 - yh])
            send(ysb.at[t, i], yrb.at[t, i], yss, ysr.at[t, i], column(0, True))

    def crossed(t, k):
        i = k % NZ
        arrived(yrb.at[t, i], ysr.at[t, i])
        return part[t, 1, zat(i), yh] + dec(0, yrb[t, i])

    def half_ring(t, d, s):
        val = crossed(t, way(d, 4 - s))
        first = 0 if d == long_way(1, t) else 1
        if s > first:
            arrived(hrb.at[t, d, s - 1], hsr.at[t, d, s - 1])
            val = val + dec(0, hrb[t, d, s - 1])
        i = slot_of(10 + t)
        hsb[t, i] = enc(0, val)
        send(hsb.at[t, i], hrb.at[t, d, s], hss, hsr.at[t, d, s], column(way(d, 1)))

    def half_total(t):
        val = crossed(t, 0)
        for d in range(2):
            arrived(hrb.at[t, d, 3], hsr.at[t, d, 3])
            val = val + dec(0, hrb[t, d, 3])
        return val

    def group(e, t, rows):
        return ag.at[e // 2, pl.ds(0, 2) if e == 2 else pl.ds(e, 1), t, rows, :]

    def gather(e, t):
        own = group(e, t, zown)
        for k, slot in ((2, 0), (1, 2)):
            for d in range(2):
                for other in (True, False):
                    send(own, own, ags, agr.at[t, e, d if k == 2 else 2], column(way(d, k), other))
        send(own, own, ags, agr.at[t, e, 2], column(0, True))

    def relay(e, t, d):
        arrived(group(e, t, pl.ds(0, 16)), agr.at[t, e, d])
        rows = group(e, t, pl.ds(pl.multiple_of(16 * zat(way(d, -2)), 16), 16))
        if d == long_way(e, t):
            send(rows, rows, ags, agr.at[t, e, 2], column(way(d, 2)))
        send(rows, rows, ags, agr.at[t, e, 2], column(way(d, 1)))

    def gathered(e, t):
        arrived(group(e, t, pl.ds(0, 88)), agr.at[t, e, 2])

    def hidden_value(t):
        val = total(t, 0, 5)
        act[t, 0] = val[0]
        act[t, 1] = val[1]
        ag[0, 0, t, zown, :] = (silu_parts(val[0])[0] * val[1]).astype(BF16)
        gather(0, t)

    def hidden_tangent(t):
        val = half_total(t)
        gate, upper, gate_dot, upper_dot = act[t, 0], act[t, 1], val[0], val[1]
        silu_val, first, second = silu_parts(gate)
        ag[0, 1, t, zown, :] = (first * gate_dot * upper + silu_val * upper_dot).astype(BF16)
        gather(1, t)
        act[t, 2] = gate_dot
        act[t, 3] = upper_dot

    def out(t, w):
        gathered(w, t)
        for n in range(0, DL, 256):
            cols = slice(n, n + 256)
            val = jnp.dot(ag[0, w, t], wdn[0, :, cols], preferred_element_type=F32)
            if w == 1:
                val = val + jnp.dot(ag[0, 0, t], wdn[1, :, cols], preferred_element_type=F32)
            osum[t, w, :, :, :, cols] = val.reshape(2, 8, 8, 256)
        osend[t, w] = encode2(osum[t, w, 1 - core])
        send(osend.at[t, w], ocore.at[t, w], oss.at[0], osr.at[0, t, w], at_gy(mate))

    def out_send(t, w):
        arrived(ocore.at[t, w], osr.at[0, t, w])
        val = osum[t, w, core] + decode2(ocore[t, w])
        osum[t, w, core] = val
        oown[t, w] = encode2(val)
        for k in far:
            dst = lax.rem(mine + k, 8)
            send(oown.at[t, w, dst], orecv.at[t, w, k], oss.at[1], osr.at[1, t, w], at_gy(2 * dst + core))

    def grads(t, w):
        arrived(orecv.at[t, w, pl.ds(1, 7)], osr.at[1, t, w])
        val = osum[t, w, core, mine]
        for k in range(1, 8):
            val = val + decode2(orecv[t, w, k])
        if w == 0:
            val = val - tgv[8 * t : 8 * t + 8, :].astype(F32)
        gs[t, w, own8, :] = (val * scale).astype(BF16)
        own = gs.at[t, w, own8, :]
        for k in all_far:
            send(own, own, gss, gsr.at[t, w], at_gy(lax.rem(h + k, NG)))

    def back(t, u):
        arrived(gs.at[t, u, pl.ds(0, 120), :], gsr.at[t, u])
        for n in range(0, FL, 256):
            m = min(256, FL - n)
            val = tail_dot(gs[t, u], wdn[0, n : n + m, :])
            if u == 1:
                val = val + tail_dot(gs[t, 0], wdn[1, n : n + m, :])
            part[t, 2, :, :, u, :, n : n + m] = val.reshape(8, 2, 8, m)
        for d in range(2):
            back_far(t, u, d, 3, 1, 0)
        back_far(t, u, (t + u) % 2, 4, 2, 1)
        for d in range(2):
            back_last(t, u, d, 1, part[t, 2, zat(way(d, 1)), :, u], 0)
        bpb[t, u] = encode2(part[t, 2, z, 1 - yh, u])
        send(bpb.at[t, u], bfin.at[t, u, 4], bpb_sem, bfin_sem.at[t, u], column(0, True))

    def back_far(t, u, d, k, hops, slot):
        i = slot_of((t, u))
        bsb[t, u, i] = encode2(part[t, 2, zat(way(d, k)), :, u])
        send(bsb.at[t, u, i], brb.at[t, u, d, slot], bsb_sem, brb_sem.at[t, u, d, slot], column(way(d, hops)))

    def back_last(t, u, d, k, val, slot):
        i = slot_of((t, u))
        bsb[t, u, i] = encode2(val)
        for other in (True, False):
            y = 1 - yh if other else yh
            dst = bfin.at[t, u, slot + d + (2 if other else 0)]
            send(bsb.at[t, u, i, y], dst, bsb_sem, bfin_sem.at[t, u], column(way(d, k), other))

    def fold(t, u, d):
        val = part[t, 2, zat(way(d, 2)), :, u]
        for slot in range(2 if d == (t + u) % 2 else 1):
            arrived(brb.at[t, u, d, slot], brb_sem.at[t, u, d, slot])
            val = val + decode2(brb[t, u, d, slot])
        back_last(t, u, d, 2, val, 5)

    def summed(t, u):
        arrived(bfin.at[t, u], bfin_sem.at[t, u])
        val = part[t, 2, z, yh, u]
        for i in range(9):
            val = val + decode2(bfin[t, u, i])
        return val

    def inner(t):
        back_val, back_dot = summed(t, 0), summed(t, 1)
        gate, upper, gate_dot, upper_dot = act[t, 0], act[t, 1], act[t, 2], act[t, 3]
        silu_val, first, second = silu_parts(gate)
        ag[1, 0, t, zown, :] = (
            back_dot * upper * first + back_val * upper_dot * first + back_val * upper * second * gate_dot
        ).astype(BF16)
        ag[1, 1, t, zown, :] = (back_dot * silu_val + back_val * first * gate_dot).astype(BF16)
        gather(2, t)

    def down(n):
        g0 = gs[:, 0, :, n : n + 256].reshape(TOKENS, 256)
        g1 = gs[:, 1, :, n : n + 256].reshape(TOKENS, 256)
        hid = ag[0, 0].reshape(TOKENS, FL)
        hid_dot = ag[0, 1].reshape(TOKENS, FL)
        hd[:, n : n + 256] = (lead_dot(hid_dot, g0) + lead_dot(hid, g1)).astype(BF16)

    def flat(t):
        xt[:, 128 * t : 128 * t + 128] = xs[t].T

    def both(f, *a):
        for d in range(2):
            f(*a, d)

    def up_waited(t, q):
        if t == 0:
            local[2 * q].wait()
            local[2 * q + 1].wait()
        up(t, q)

    def out_waited(t, w):
        if t == 0:
            local[4 + w].wait()
        if t == 0 and w == 0:
            own_tgt.wait()
        out(t, w)

    def half_way(t, short, s):
        half_ring(t, (long_way(1, t) + short) % 2, s)

    def full_way(t, short, s):
        ring(t, 0, (long_way(0, t) + short) % 2, s)

    steps = {
        "up": up_waited,
        "cross0": lambda t: cross(t, (4, -3, 3)),
        "cross1": lambda t: cross(t, (2, -2, 1, -1, 0)),
        "start": ring_start,
        "half": half_way,
        "full": full_way,
        "hidden": hidden_value,
        "hiddent": hidden_tangent,
        "pass": lambda t: both(relay, 0, t),
        "passt": lambda t: both(relay, 1, t),
        "out": out_waited,
        "outs": out_send,
        "grads": grads,
        "back": back,
        "fold": lambda t, u: both(fold, t, u),
        "inner": inner,
        "pass1": lambda t: both(relay, 2, t),
        "down": down,
        "flat": flat,
    }
    for name, *a in ORDER:
        with jax.named_scope(name + "_".join(str(i) for i in a)):
            steps[name](*a)
    xt_copy = local_copy(xt, xt_out, 9)
    hd_copy = local_copy(hd, hd_out, 10)
    for t in range(2):
        with jax.named_scope("gathered%d" % t):
            gathered(2, t)
    with jax.named_scope("tail"):
        ag_copy = local_copy(ag.at[1], ag_out, 11)
        left(xs.at[:, pl.ds(0, 120), :], xsem.at[0])
        left(sbuf, rss)
        left(pbuf, pss)
        left(ysb, yss)
        left(hsb, hss)
        left(bsb, bsb_sem)
        left(bpb, bpb_sem)
        left(ag.at[:, :, :, pl.ds(0, 120), :], ags)
        left(osend, oss.at[0])
        left(oown.at[:, :, pl.ds(0, 7)], oss.at[1])
        left(gs.at[:, :, pl.ds(0, 120), :], gss)
        xt_copy.wait()
        hd_copy.wait()
        ag_copy.wait()


def weights_kernel(xt, ag, hd, gate_out, up_out, down_out, buf, sem):
    rows = DL // 4
    down = pltpu.make_async_copy(hd, down_out, sem.at[8])
    down.start()
    copies = []
    for v, out in enumerate((gate_out, up_out)):
        for i in range(4):
            part = pl.ds(i * rows, rows)
            buf[v, part, :] = jnp.dot(xt[part, :], ag[v], preferred_element_type=F32).astype(BF16)
            copy = pltpu.make_async_copy(buf.at[v, part, :], out.at[part, :], sem.at[4 * v + i])
            copy.start()
            copies.append(copy)
    down.wait()
    for copy in copies:
        copy.wait()


def body(*args):
    hbm = pl.BlockSpec(memory_space=pltpu.HBM)
    vmem = pl.BlockSpec(memory_space=pltpu.VMEM)
    dma = pltpu.SemaphoreType.DMA
    args = [pltpu.with_memory_space_constraint(a, pltpu.HBM) for a in args]
    xt, ag, hd = pl.pallas_call(
        kernel,
        out_shape=(
            jax.ShapeDtypeStruct((DL, TOKENS), BF16),
            jax.ShapeDtypeStruct((2, 2, 128, FL), BF16),
            jax.ShapeDtypeStruct((FL, DL), BF16),
        ),
        in_specs=[hbm] * 8,
        out_specs=(pl.BlockSpec(memory_space=pl.ANY),) * 3,
        scratch_shapes=[
            pltpu.VMEM((2, 128, DL), BF16),
            pltpu.VMEM((DL, TOKENS), BF16),
            pltpu.VMEM((FL, DL), BF16),
            pltpu.VMEM((TOKENS // NG, DL), BF16),
            pltpu.VMEM((4, DL, FL), BF16),
            pltpu.VMEM((2, FL, DL), BF16),
            pltpu.VMEM((2, 3, 8, 2, 2, 8, FL), F32),
            pltpu.VMEM((2, 7, 2, 2, 8, FL), BF16),
            pltpu.VMEM((2, 2, 3, 2, 2, 8, FL), BF16),
            pltpu.VMEM((2, 2, 8, FL), BF16),
            pltpu.VMEM((2, 5, 2, 8, FL), BF16),
            pltpu.VMEM((2, 8, 2, 8, FL), BF16),
            pltpu.VMEM((2, 8, 2, 8, FL), BF16),
            pltpu.VMEM((2, 7, 2, 8, FL), BF16),
            pltpu.VMEM((2, 2, 4, 2, 8, FL), BF16),
            pltpu.VMEM((2, 2, 7, 2, 8, FL), BF16),
            pltpu.VMEM((2, 2, 2, 2, 2, 8, FL), BF16),
            pltpu.VMEM((2, 2, 8, FL), BF16),
            pltpu.VMEM((2, 2, 9, 8, FL), BF16),
            pltpu.VMEM((2, 4, 8, FL), F32),
            pltpu.VMEM((2, 2, 2, 128, FL), BF16),
            pltpu.VMEM((2, 2, 2, 8, 8, DL), F32),
            pltpu.VMEM((2, 2, 8, 8, DL), BF16),
            pltpu.VMEM((2, 2, 8, 8, DL), BF16),
            pltpu.VMEM((2, 2, 8, 8, DL), BF16),
            pltpu.VMEM((2, 2, 8, 8, DL), BF16),
            pltpu.VMEM((2, 2, 128, DL), BF16),
            dma((12,)),
            dma((4,)),
            dma, dma,
            dma((2, 2, 3)),
            dma((2,)),
            dma, dma((2, 8)),
            dma, dma((2, 2, 4)),
            dma, dma((2, 2, 2, 2)), dma, dma((2, 2)),
            dma,
            dma((2, 3, 3)),
            dma((2,)), dma((2, 2, 2)),
            dma, dma((2, 2)),
        ],
        compiler_params=pltpu.CompilerParams(
            collective_id=0, has_side_effects=True, vmem_limit_bytes=40 * 1024 * 1024
        ),
    )(*args)
    return pl.pallas_call(
        weights_kernel,
        out_shape=(
            jax.ShapeDtypeStruct((DL, FL), BF16),
            jax.ShapeDtypeStruct((DL, FL), BF16),
            jax.ShapeDtypeStruct((FL, DL), BF16),
        ),
        in_specs=[vmem] * 3,
        out_specs=(hbm,) * 3,
        scratch_shapes=[pltpu.VMEM((2, DL, FL), BF16), dma((9,))],
        compiler_params=pltpu.CompilerParams(vmem_limit_bytes=16 * 1024 * 1024),
    )(xt, ag.reshape(2, TOKENS, FL), hd)


def solution(mesh):
    in_specs = (
        P("gy", "gx"),
        P("gy", "gx"),
        P("gx", "gy"),
        P("gx", "gy"),
        P("gy", "gx"),
        P("gx", "gy"),
        P("gx", "gy"),
        P("gy", "gx"),
    )
    out_specs = (P("gx", "gy"), P("gx", "gy"), P("gy", "gx"))
    return jax.shard_map(body, mesh=mesh, in_specs=in_specs, out_specs=out_specs, check_vma=False)
```

```python
import functools
import math

import jax
import jax.numpy as jnp
from jax import lax
from jax.experimental import pallas as pl
from jax.experimental.pallas import tpu as pltpu
from jax.sharding import PartitionSpec as P

MESH = pl.DeviceIdType.MESH
TOKENS = 256
DL = 512
FL = 896
NZ = 8
NG = 16
F32 = jnp.float32
BF16 = jnp.bfloat16


def silu_parts(gate):
    sig = jax.nn.sigmoid(gate)
    first = sig * (1.0 + gate * (1.0 - sig))
    second = sig * (1.0 - sig) * (2.0 + gate * (1.0 - 2.0 * sig))
    return (gate * sig, first, second)


def lead_dot(left, right):
    return lax.dot_general(left, right, (((0,), (0,)), ((), ())), preferred_element_type=F32)


def tail_dot(left, right):
    return lax.dot_general(left, right, (((1,), (1,)), ((), ())), preferred_element_type=F32)


TINY = 1e-36


def encode2(v):
    return (v * jnp.abs(v)).astype(BF16)


def decode2(c):
    v = c.astype(F32)
    return v * lax.rsqrt(jnp.maximum(jnp.abs(v), TINY))


def encode4(v):
    return (v * jnp.abs(v) * (v * v)).astype(BF16)


def decode4(c):
    v = c.astype(F32)
    w = lax.rsqrt(jnp.maximum(jnp.abs(v), TINY))
    return v * w * (w * lax.rsqrt(w))


ORDER = (
    ("up", 0, 1), ("cross0", 0), ("up", 0, 0), ("start", 0), ("up", 1, 1), ("cross0", 1), ("cross1", 0), ("up", 1, 0), ("start", 1), ("cross1", 1),
    ("full", 0, 0, 1), ("half", 0, 0, 0), ("half", 0, 1, 1), ("full", 1, 0, 1), ("half", 1, 0, 0), ("half", 1, 1, 1), ("full", 0, 0, 2),
    ("full", 0, 1, 2), ("half", 0, 0, 1), ("full", 1, 0, 2), ("full", 1, 1, 2), ("half", 1, 0, 1), ("full", 0, 0, 3), ("full", 0, 1, 3),
    ("half", 0, 0, 2), ("half", 0, 1, 2), ("full", 1, 0, 3), ("full", 1, 1, 3), ("half", 1, 0, 2), ("half", 1, 1, 2), ("flat", 0), ("flat", 1),
    ("hidden", 0), ("half", 0, 0, 3), ("half", 0, 1, 3), ("hidden", 1), ("half", 1, 0, 3), ("half", 1, 1, 3), ("hiddent", 0), ("hiddent", 1),
    ("pass", 0), ("pass", 1), ("passt", 0), ("passt", 1), ("out", 0, 0), ("out", 1, 0), ("outs", 0, 0), ("outs", 1, 0), ("out", 0, 1), ("out", 1, 1),
    ("outs", 0, 1), ("outs", 1, 1), ("grads", 0, 0), ("grads", 1, 0), ("grads", 0, 1), ("grads", 1, 1), ("back", 0, 0), ("back", 1, 0),
    ("back", 0, 1), ("back", 1, 1), ("down", 0), ("down", 256), ("fold", 0, 0), ("fold", 1, 0), ("fold", 0, 1), ("fold", 1, 1), ("inner", 0),
    ("inner", 1), ("pass1", 0), ("pass1", 1),
)


def kernel(
    tok, tgt, wg, wu, wd, tg, tu, td,
    xt_out, ag_out, hd_out,
    xs, xt, hd, tgv, wup, wdn, part, sbuf, rbuf, pbuf, fin, ysb, yrb, hsb, hrb, bsb, brb, bpb, bfin, act, ag, osum, osend, ocore, oown, orecv, gs,
    lsem, xsem, rss, pss, rsr, fsr, yss, ysr, hss, hsr, bsb_sem, brb_sem, bpb_sem, bfin_sem, ags, agr, oss, osr, gss, gsr,
):
    scale = 1.0 / math.sqrt(TOKENS)
    g = lax.axis_index("gx")
    h = lax.axis_index("gy")
    core = lax.rem(h, 2)
    mine = lax.div(h, 2)
    mate = h + 1 - 2 * core
    yh = lax.div(g, NZ)
    z = lax.rem(g, NZ)
    own8 = pl.ds(pl.multiple_of(64 * core + 8 * mine, 8), 8)
    core64 = pl.ds(pl.multiple_of(64 * core, 64), 64)
    zown = pl.ds(pl.multiple_of(16 * z + 8 * yh, 8), 8)

    def zat(k):
        return lax.rem(z + k + NZ, NZ)

    def column(k, other=False):
        y = 1 - yh if other else yh
        return {"gx": y * NZ + zat(k)}

    def at_gy(i):
        return {"gy": i}

    def way(d, k):
        return k if d == 0 else -k

    def send(src, dst, ssem, rsem, where):
        pltpu.make_async_remote_copy(
            src_ref=src, dst_ref=dst, send_sem=ssem, recv_sem=rsem, device_id=where, device_id_type=MESH
        ).start()

    def arrived(ref, sem):
        pltpu.make_async_remote_copy(
            src_ref=ref, dst_ref=ref, send_sem=sem, recv_sem=sem, device_id=at_gy(mate), device_id_type=MESH
        ).wait_recv()

    def left(ref, sem):
        pltpu.make_async_remote_copy(
            src_ref=ref, dst_ref=ref, send_sem=sem, recv_sem=sem, device_id=at_gy(mate), device_id_type=MESH
        ).wait_send()

    def local_copy(src, dst, i):
        copy = pltpu.make_async_copy(src, dst, lsem.at[i])
        copy.start()
        return copy

    own_tok = [local_copy(tok.at[pl.ds(8 * t, 8), :], xs.at[t, own8, :], t) for t in range(2)]
    local = [local_copy(w, wup.at[i], 2 + i) for i, w in enumerate((wg, wu, tg, tu))]
    local += [local_copy(w, wdn.at[i], 6 + i) for i, w in enumerate((wd, td))]
    own_tgt = local_copy(tgt, tgv, 8)

    with jax.named_scope("barrier"):
        barrier = pltpu.get_barrier_semaphore()
        near = [column(k, o) for k in (1, -1, 2, -2) for o in (False, True)] + [column(0, True)]
        near += [at_gy(lax.rem(h + k, NG)) for k in range(1, NG)]
        for where in near:
            pl.semaphore_signal(barrier, inc=1, device_id=where, device_id_type=MESH)
        pl.semaphore_wait(barrier, len(near))

    far = (4, 5, 3, 6, 2, 7, 1)
    all_far = (8, 10, 6, 9, 7, 11, 5, 12, 4, 14, 2, 13, 3, 15, 1)

    with jax.named_scope("tokens"):
        for c in own_tok:
            c.wait()
        for k in all_far:
            send(xs.at[:, own8, :], xs.at[:, own8, :], xsem.at[0], xsem.at[1], at_gy(lax.rem(h + k, NG)))
        arrived(xs.at[:, pl.ds(0, 120), :], xsem.at[1])

    slots = {}

    def slot_of(tq):
        slots[tq] = slots.get(tq, -1) + 1
        return slots[tq]

    def enc(q, v):
        return encode4(v) if q < 2 else encode2(v)

    def dec(q, v):
        return decode4(v) if q < 2 else decode2(v)

    def long_way(q, t):
        return (q + t) % 2

    def chunk(t, q, d, k):
        return part[t, q, zat(way(d, k))]

    def send_whole(t, q, val, d, hops, slot):
        tq = t
        i = slot_of(tq)
        sbuf[tq, i] = enc(q, val)
        send(sbuf.at[tq, i], rbuf.at[tq, d, slot], rss, rsr.at[tq, d, slot], column(way(d, hops)))

    def send_last(t, q, val, d, hops, slot):
        tq = t
        i = slot_of(tq)
        sbuf[tq, i] = enc(q, val)
        for other in (True, False):
            y = 1 - yh if other else yh
            dst = fin.at[tq, slot + d + (2 if other else 0)]
            send(sbuf.at[tq, i, y], dst, rss, fsr.at[tq], column(way(d, hops), other))

    def send_pair(t, q):
        tq = t
        pbuf[tq] = enc(q, part[t, q, z, 1 - yh])
        send(pbuf.at[tq], fin.at[tq, 4], pss, fsr.at[tq], column(0, True))

    def taken(t, q, d, slot):
        tq = t
        arrived(rbuf.at[tq, d, slot], rsr.at[tq, d, slot])
        return dec(q, rbuf[tq, d, slot])

    def total(t, q, n):
        tq = t
        arrived(fin.at[tq, pl.ds(0, n)], fsr.at[tq])
        val = part[t, q, z, yh]
        for i in range(n):
            val = val + dec(q, fin[tq, i])
        return val

    def up(t, q):
        for u in range(2):
            for n in range(0, FL, 256):
                m = min(256, FL - n)
                val = jnp.dot(xs[t], wup[2 * q + u, :, n : n + m], preferred_element_type=F32)
                part[t, q, :, :, u, :, n : n + m] = val.reshape(8, 2, 8, m)

    def ring_start(t):
        d = long_way(0, t)
        send_whole(t, 0, chunk(t, 0, d, 4), d, 1, 0)
        send_whole(t, 0, chunk(t, 0, 1 - d, 3), 1 - d, 1, 1)
        send_pair(t, 0)

    def ring(t, q, d, s):
        val = chunk(t, q, d, 4 - s) + taken(t, q, d, s - 1)
        if s < 3:
            send_whole(t, q, val, d, 1, s)
        else:
            send_last(t, q, val, d, 1, 0)

    waited = set()

    def cross_group(i):
        return {4: 0, 3: 0, 5: 0, 2: 1, 6: 1}.get(i, 2)

    def cross(t, ks):
        d = long_way(1, t)
        for k in ks:
            i = way(d, k) % NZ
            ysb[t, i] = enc(0, part[t, 1, zat(i), 1 - yh])
            send(ysb.at[t, i], yrb.at[t, i], yss, ysr.at[t, cross_group(i)], column(0, True))

    def crossed(t, k):
        i = k % NZ
        e = cross_group(i)
        if (t, e) not in waited:
            waited.add((t, e))
            arrived(yrb.at[t, pl.ds(0, 2 if e == 1 else 3)], ysr.at[t, e])
        return part[t, 1, zat(i), yh] + dec(0, yrb[t, i])

    def half_ring(t, d, s):
        val = crossed(t, way(d, 4 - s))
        first = 0 if d == long_way(1, t) else 1
        if s > first:
            arrived(hrb.at[t, d, s - 1], hsr.at[t, d, s - 1])
            val = val + dec(0, hrb[t, d, s - 1])
        i = slot_of(10 + t)
        hsb[t, i] = enc(0, val)
        send(hsb.at[t, i], hrb.at[t, d, s], hss, hsr.at[t, d, s], column(way(d, 1)))

    def half_total(t):
        val = crossed(t, 0)
        for d in range(2):
            arrived(hrb.at[t, d, 3], hsr.at[t, d, 3])
            val = val + dec(0, hrb[t, d, 3])
        return val

    def group(e, t, rows):
        return ag.at[e // 2, pl.ds(0, 2) if e == 2 else pl.ds(e, 1), t, rows, :]

    def gather(e, t):
        own = group(e, t, zown)
        for k, slot in ((2, 0), (1, 2)):
            for d in range(2):
                for other in (True, False):
                    send(own, own, ags, agr.at[t, e, d if k == 2 else 2], column(way(d, k), other))
        send(own, own, ags, agr.at[t, e, 2], column(0, True))

    def relay(e, t, d):
        arrived(group(e, t, pl.ds(0, 16)), agr.at[t, e, d])
        rows = group(e, t, pl.ds(pl.multiple_of(16 * zat(way(d, -2)), 16), 16))
        if d == long_way(e, t):
            send(rows, rows, ags, agr.at[t, e, 2], column(way(d, 2)))
        send(rows, rows, ags, agr.at[t, e, 2], column(way(d, 1)))

    def gathered(e, t):
        arrived(group(e, t, pl.ds(0, 88)), agr.at[t, e, 2])

    def hidden_value(t):
        val = total(t, 0, 5)
        act[t, 0] = val[0]
        act[t, 1] = val[1]
        ag[0, 0, t, zown, :] = (silu_parts(val[0])[0] * val[1]).astype(BF16)
        gather(0, t)

    def hidden_tangent(t):
        val = half_total(t)
        gate, upper, gate_dot, upper_dot = act[t, 0], act[t, 1], val[0], val[1]
        silu_val, first, second = silu_parts(gate)
        ag[0, 1, t, zown, :] = (first * gate_dot * upper + silu_val * upper_dot).astype(BF16)
        gather(1, t)
        act[t, 2] = gate_dot
        act[t, 3] = upper_dot

    def out(t, w):
        gathered(w, t)
        for n in range(0, DL, 256):
            cols = slice(n, n + 256)
            val = jnp.dot(ag[0, w, t], wdn[0, :, cols], preferred_element_type=F32)
            if w == 1:
                val = val + jnp.dot(ag[0, 0, t], wdn[1, :, cols], preferred_element_type=F32)
            osum[t, w, :, :, :, cols] = val.reshape(2, 8, 8, 256)
        osend[t, w] = encode2(osum[t, w, 1 - core])
        send(osend.at[t, w], ocore.at[t, w], oss.at[0], osr.at[0, t, w], at_gy(mate))

    def out_send(t, w):
        arrived(ocore.at[t, w], osr.at[0, t, w])
        val = osum[t, w, core] + decode2(ocore[t, w])
        osum[t, w, core] = val
        oown[t, w] = encode2(val)
        for k in far:
            dst = lax.rem(mine + k, 8)
            send(oown.at[t, w, dst], orecv.at[t, w, k], oss.at[1], osr.at[1, t, w], at_gy(2 * dst + core))

    def grads(t, w):
        arrived(orecv.at[t, w, pl.ds(1, 7)], osr.at[1, t, w])
        val = osum[t, w, core, mine]
        for k in range(1, 8):
            val = val + decode2(orecv[t, w, k])
        if w == 0:
            val = val - tgv[8 * t : 8 * t + 8, :].astype(F32)
        gs[t, w, own8, :] = (val * scale).astype(BF16)
        own = gs.at[t, w, own8, :]
        for k in all_far:
            send(own, own, gss, gsr.at[t, w], at_gy(lax.rem(h + k, NG)))

    def back(t, u):
        arrived(gs.at[t, u, pl.ds(0, 120), :], gsr.at[t, u])
        for n in range(0, FL, 256):
            m = min(256, FL - n)
            val = tail_dot(gs[t, u], wdn[0, n : n + m, :])
            if u == 1:
                val = val + tail_dot(gs[t, 0], wdn[1, n : n + m, :])
            part[t, 2, :, :, u, :, n : n + m] = val.reshape(8, 2, 8, m)
        for d in range(2):
            back_far(t, u, d, 3, 1, 0)
        back_far(t, u, (t + u) % 2, 4, 2, 1)
        for d in range(2):
            back_last(t, u, d, 1, part[t, 2, zat(way(d, 1)), :, u], 0)
        bpb[t, u] = encode2(part[t, 2, z, 1 - yh, u])
        send(bpb.at[t, u], bfin.at[t, u, 4], bpb_sem, bfin_sem.at[t, u], column(0, True))

    def back_far(t, u, d, k, hops, slot):
        i = slot_of((t, u))
        bsb[t, u, i] = encode2(part[t, 2, zat(way(d, k)), :, u])
        send(bsb.at[t, u, i], brb.at[t, u, d, slot], bsb_sem, brb_sem.at[t, u, 2 if slot else d], column(way(d, hops)))

    def back_last(t, u, d, k, val, slot):
        i = slot_of((t, u))
        bsb[t, u, i] = encode2(val)
        for other in (True, False):
            y = 1 - yh if other else yh
            dst = bfin.at[t, u, slot + d + (2 if other else 0)]
            send(bsb.at[t, u, i, y], dst, bsb_sem, bfin_sem.at[t, u], column(way(d, k), other))

    def fold(t, u, d):
        val = part[t, 2, zat(way(d, 2)), :, u]
        for slot in range(2 if d == (t + u) % 2 else 1):
            arrived(brb.at[t, u, d, slot], brb_sem.at[t, u, 2 if slot else d])
            val = val + decode2(brb[t, u, d, slot])
        back_last(t, u, d, 2, val, 5)

    def summed(t, u):
        arrived(bfin.at[t, u], bfin_sem.at[t, u])
        val = part[t, 2, z, yh, u]
        for i in range(9):
            val = val + decode2(bfin[t, u, i])
        return val

    def inner(t):
        back_val, back_dot = summed(t, 0), summed(t, 1)
        gate, upper, gate_dot, upper_dot = act[t, 0], act[t, 1], act[t, 2], act[t, 3]
        silu_val, first, second = silu_parts(gate)
        ag[1, 0, t, zown, :] = (
            back_dot * upper * first + back_val * upper_dot * first + back_val * upper * second * gate_dot
        ).astype(BF16)
        ag[1, 1, t, zown, :] = (back_dot * silu_val + back_val * first * gate_dot).astype(BF16)
        gather(2, t)

    def down(n):
        g0 = gs[:, 0, :, n : n + 256].reshape(TOKENS, 256)
        g1 = gs[:, 1, :, n : n + 256].reshape(TOKENS, 256)
        hid = ag[0, 0].reshape(TOKENS, FL)
        hid_dot = ag[0, 1].reshape(TOKENS, FL)
        hd[:, n : n + 256] = (lead_dot(hid_dot, g0) + lead_dot(hid, g1)).astype(BF16)

    def flat(t):
        xt[:, 128 * t : 128 * t + 128] = xs[t].T

    def both(f, *a):
        for d in range(2):
            f(*a, d)

    def up_waited(t, q):
        if t == 0:
            local[2 * q].wait()
            local[2 * q + 1].wait()
        up(t, q)

    def out_waited(t, w):
        if t == 0:
            local[4 + w].wait()
        if t == 0 and w == 0:
            own_tgt.wait()
        out(t, w)

    def half_way(t, short, s):
        half_ring(t, (long_way(1, t) + short) % 2, s)

    def full_way(t, short, s):
        ring(t, 0, (long_way(0, t) + short) % 2, s)

    steps = {
        "up": up_waited,
        "cross0": lambda t: cross(t, (4, -3, 3)),
        "cross1": lambda t: cross(t, (2, -2, 1, -1, 0)),
        "start": ring_start,
        "half": half_way,
        "full": full_way,
        "hidden": hidden_value,
        "hiddent": hidden_tangent,
        "pass": lambda t: both(relay, 0, t),
        "passt": lambda t: both(relay, 1, t),
        "out": out_waited,
        "outs": out_send,
        "grads": grads,
        "back": back,
        "fold": lambda t, u: both(fold, t, u),
        "inner": inner,
        "pass1": lambda t: both(relay, 2, t),
        "down": down,
        "flat": flat,
    }
    for name, *a in ORDER:
        with jax.named_scope(name + "_".join(str(i) for i in a)):
            steps[name](*a)
    xt_copy = local_copy(xt, xt_out, 2)
    hd_copy = local_copy(hd, hd_out, 3)
    ag_copies = []
    for t in range(2):
        with jax.named_scope("gathered%d" % t):
            gathered(2, t)
            ag_copies.append(local_copy(ag.at[1, :, t], ag_out.at[:, t], t))
    with jax.named_scope("tail"):
        left(xs.at[:, pl.ds(0, 120), :], xsem.at[0])
        left(sbuf, rss)
        left(pbuf, pss)
        left(ysb, yss)
        left(hsb, hss)
        left(bsb, bsb_sem)
        left(bpb, bpb_sem)
        left(ag.at[:, :, :, pl.ds(0, 120), :], ags)
        left(osend, oss.at[0])
        left(oown.at[:, :, pl.ds(0, 7)], oss.at[1])
        left(gs.at[:, :, pl.ds(0, 120), :], gss)
        xt_copy.wait()
        hd_copy.wait()
        for c in ag_copies:
            c.wait()


def weights_kernel(xt, ag, hd, gate_out, up_out, down_out, buf, sem):
    rows = DL // 4
    down = pltpu.make_async_copy(hd, down_out, sem.at[8])
    down.start()
    copies = []
    for v, out in enumerate((gate_out, up_out)):
        for i in range(4):
            part = pl.ds(i * rows, rows)
            buf[v, part, :] = jnp.dot(xt[part, :], ag[v], preferred_element_type=F32).astype(BF16)
            copy = pltpu.make_async_copy(buf.at[v, part, :], out.at[part, :], sem.at[4 * v + i])
            copy.start()
            copies.append(copy)
    down.wait()
    for copy in copies:
        copy.wait()


def body(*args):
    hbm = pl.BlockSpec(memory_space=pltpu.HBM)
    vmem = pl.BlockSpec(memory_space=pltpu.VMEM)
    dma = pltpu.SemaphoreType.DMA
    args = [pltpu.with_memory_space_constraint(a, pltpu.HBM) for a in args]
    xt, ag, hd = pl.pallas_call(
        kernel,
        out_shape=(
            jax.ShapeDtypeStruct((DL, TOKENS), BF16),
            jax.ShapeDtypeStruct((2, 2, 128, FL), BF16),
            jax.ShapeDtypeStruct((FL, DL), BF16),
        ),
        in_specs=[hbm] * 8,
        out_specs=(pl.BlockSpec(memory_space=pl.ANY),) * 3,
        scratch_shapes=[
            pltpu.VMEM((2, 128, DL), BF16),
            pltpu.VMEM((DL, TOKENS), BF16),
            pltpu.VMEM((FL, DL), BF16),
            pltpu.VMEM((TOKENS // NG, DL), BF16),
            pltpu.VMEM((4, DL, FL), BF16),
            pltpu.VMEM((2, FL, DL), BF16),
            pltpu.VMEM((2, 3, 8, 2, 2, 8, FL), F32),
            pltpu.VMEM((2, 7, 2, 2, 8, FL), BF16),
            pltpu.VMEM((2, 2, 3, 2, 2, 8, FL), BF16),
            pltpu.VMEM((2, 2, 8, FL), BF16),
            pltpu.VMEM((2, 5, 2, 8, FL), BF16),
            pltpu.VMEM((2, 8, 2, 8, FL), BF16),
            pltpu.VMEM((2, 8, 2, 8, FL), BF16),
            pltpu.VMEM((2, 7, 2, 8, FL), BF16),
            pltpu.VMEM((2, 2, 4, 2, 8, FL), BF16),
            pltpu.VMEM((2, 2, 7, 2, 8, FL), BF16),
            pltpu.VMEM((2, 2, 2, 2, 2, 8, FL), BF16),
            pltpu.VMEM((2, 2, 8, FL), BF16),
            pltpu.VMEM((2, 2, 9, 8, FL), BF16),
            pltpu.VMEM((2, 4, 8, FL), F32),
            pltpu.VMEM((2, 2, 2, 128, FL), BF16),
            pltpu.VMEM((2, 2, 2, 8, 8, DL), F32),
            pltpu.VMEM((2, 2, 8, 8, DL), BF16),
            pltpu.VMEM((2, 2, 8, 8, DL), BF16),
            pltpu.VMEM((2, 2, 8, 8, DL), BF16),
            pltpu.VMEM((2, 2, 8, 8, DL), BF16),
            pltpu.VMEM((2, 2, 128, DL), BF16),
            dma((9,)),
            dma((2,)),
            dma, dma,
            dma((2, 2, 3)),
            dma((2,)),
            dma, dma((2, 3)),
            dma, dma((2, 2, 4)),
            dma, dma((2, 2, 3)), dma, dma((2, 2)),
            dma,
            dma((2, 3, 3)),
            dma((2,)), dma((2, 2, 2)),
            dma, dma((2, 2)),
        ],
        compiler_params=pltpu.CompilerParams(
            collective_id=0, has_side_effects=True, vmem_limit_bytes=40 * 1024 * 1024
        ),
    )(*args)
    return pl.pallas_call(
        weights_kernel,
        out_shape=(
            jax.ShapeDtypeStruct((DL, FL), BF16),
            jax.ShapeDtypeStruct((DL, FL), BF16),
            jax.ShapeDtypeStruct((FL, DL), BF16),
        ),
        in_specs=[vmem] * 3,
        out_specs=(hbm,) * 3,
        scratch_shapes=[pltpu.VMEM((2, DL, FL), BF16), dma((9,))],
        compiler_params=pltpu.CompilerParams(vmem_limit_bytes=16 * 1024 * 1024),
    )(xt, ag.reshape(2, TOKENS, FL), hd)


def solution(mesh):
    in_specs = (
        P("gy", "gx"),
        P("gy", "gx"),
        P("gx", "gy"),
        P("gx", "gy"),
        P("gy", "gx"),
        P("gx", "gy"),
        P("gx", "gy"),
        P("gy", "gx"),
    )
    out_specs = (P("gx", "gy"), P("gx", "gy"), P("gy", "gx"))
    return jax.shard_map(body, mesh=mesh, in_specs=in_specs, out_specs=out_specs, check_vma=False)
```

```python
import functools
import math

import jax
import jax.numpy as jnp
from jax import lax
from jax.experimental import pallas as pl
from jax.experimental.pallas import tpu as pltpu
from jax.sharding import PartitionSpec as P

MESH = pl.DeviceIdType.MESH
TOKENS = 256
DL = 512
FL = 896
NZ = 8
NG = 16
F32 = jnp.float32
BF16 = jnp.bfloat16


def silu_parts(gate):
    sig = jax.nn.sigmoid(gate)
    first = sig * (1.0 + gate * (1.0 - sig))
    second = sig * (1.0 - sig) * (2.0 + gate * (1.0 - 2.0 * sig))
    return (gate * sig, first, second)


def lead_dot(left, right):
    return lax.dot_general(left, right, (((0,), (0,)), ((), ())), preferred_element_type=F32)


def tail_dot(left, right):
    return lax.dot_general(left, right, (((1,), (1,)), ((), ())), preferred_element_type=F32)


TINY = 1e-36


def encode2(v):
    return (v * jnp.abs(v)).astype(BF16)


def decode2(c):
    v = c.astype(F32)
    return v * lax.rsqrt(jnp.maximum(jnp.abs(v), TINY))


def encode4(v):
    return (v * jnp.abs(v) * (v * v)).astype(BF16)


def decode4(c):
    v = c.astype(F32)
    w = lax.rsqrt(jnp.maximum(jnp.abs(v), TINY))
    return v * w * (w * lax.rsqrt(w))


ORDER = (
    ("up", 0, 1), ("cross0", 0), ("up", 0, 0), ("start", 0), ("up", 1, 1), ("cross0", 1), ("cross1", 0), ("up", 1, 0), ("start", 1), ("cross1", 1),
    ("full", 0, 0, 1), ("half", 0, 0, 0), ("half", 0, 1, 1), ("full", 1, 0, 1), ("half", 1, 0, 0), ("half", 1, 1, 1), ("full", 0, 0, 2),
    ("full", 0, 1, 2), ("half", 0, 0, 1), ("full", 1, 0, 2), ("full", 1, 1, 2), ("half", 1, 0, 1), ("full", 0, 0, 3), ("full", 0, 1, 3),
    ("half", 0, 0, 2), ("half", 0, 1, 2), ("full", 1, 0, 3), ("full", 1, 1, 3), ("half", 1, 0, 2), ("half", 1, 1, 2), ("flat", 0), ("flat", 1),
    ("hidden", 0), ("half", 0, 0, 3), ("half", 0, 1, 3), ("hidden", 1), ("half", 1, 0, 3), ("half", 1, 1, 3), ("hiddent", 0), ("hiddent", 1),
    ("pass", 0), ("pass", 1), ("passt", 0), ("passt", 1), ("out", 0, 0), ("out", 1, 0), ("outs", 0, 0), ("outs", 1, 0), ("out", 0, 1), ("out", 1, 1),
    ("outs", 0, 1), ("outs", 1, 1), ("grads", 0, 0), ("grads", 1, 0), ("grads", 0, 1), ("grads", 1, 1), ("back", 0, 0), ("back", 1, 0),
    ("back", 0, 1), ("back", 1, 1), ("down", 0), ("down", 256), ("fold", 0, 0), ("fold", 1, 0), ("fold", 0, 1), ("fold", 1, 1), ("inner", 0),
    ("inner", 1), ("pass1", 0), ("pass1", 1),
)


def kernel(
    tok, tgt, wg, wu, wd, tg, tu, td,
    xt_out, ag_out, hd_out,
    xs, xt, hd, tgv, wup, wdn, part, sbuf, rbuf, pbuf, fin, ysb, yrb, hsb, hrb, bsb, brb, bpb, bfin, act, ag, osum, osend, ocore, oown, orecv, gs,
    lsem, xsem, rss, pss, rsr, fsr, yss, ysr, hss, hsr, bsb_sem, brb_sem, bpb_sem, bfin_sem, ags, agr, oss, osr, gss, gsr,
):
    scale = 1.0 / math.sqrt(TOKENS)
    g = lax.axis_index("gx")
    h = lax.axis_index("gy")
    core = lax.rem(h, 2)
    mine = lax.div(h, 2)
    mate = h + 1 - 2 * core
    yh = lax.div(g, NZ)
    z = lax.rem(g, NZ)
    own8 = pl.ds(pl.multiple_of(64 * core + 8 * mine, 8), 8)
    core64 = pl.ds(pl.multiple_of(64 * core, 64), 64)
    zown = pl.ds(pl.multiple_of(16 * z + 8 * yh, 8), 8)

    def zat(k):
        return lax.rem(z + k + NZ, NZ)

    def column(k, other=False):
        y = 1 - yh if other else yh
        return {"gx": y * NZ + zat(k)}

    def at_gy(i):
        return {"gy": i}

    def way(d, k):
        return k if d == 0 else -k

    def send(src, dst, ssem, rsem, where):
        pltpu.make_async_remote_copy(
            src_ref=src, dst_ref=dst, send_sem=ssem, recv_sem=rsem, device_id=where, device_id_type=MESH
        ).start()

    def arrived(ref, sem):
        pltpu.make_async_remote_copy(
            src_ref=ref, dst_ref=ref, send_sem=sem, recv_sem=sem, device_id=at_gy(mate), device_id_type=MESH
        ).wait_recv()

    def left(ref, sem):
        pltpu.make_async_remote_copy(
            src_ref=ref, dst_ref=ref, send_sem=sem, recv_sem=sem, device_id=at_gy(mate), device_id_type=MESH
        ).wait_send()

    def local_copy(src, dst, i):
        copy = pltpu.make_async_copy(src, dst, lsem.at[i])
        copy.start()
        return copy

    own_tok = [local_copy(tok.at[pl.ds(8 * t, 8), :], xs.at[t, own8, :], t) for t in range(2)]
    local = [local_copy(w, wup.at[i], 2 + i) for i, w in enumerate((wg, wu, tg, tu))]
    local += [local_copy(w, wdn.at[i], 6 + i) for i, w in enumerate((wd, td))]
    own_tgt = local_copy(tgt, tgv, 8)

    with jax.named_scope("barrier"):
        barrier = pltpu.get_barrier_semaphore()
        near = [column(k, o) for k in (1, -1, 2, -2) for o in (False, True)] + [column(0, True)]
        near += [at_gy(lax.rem(h + k, NG)) for k in range(1, NG)]
        for where in near:
            pl.semaphore_signal(barrier, inc=1, device_id=where, device_id_type=MESH)
        pl.semaphore_wait(barrier, len(near))

    far = (4, 5, 3, 6, 2, 7, 1)
    all_far = (8, 10, 6, 9, 7, 11, 5, 12, 4, 14, 2, 13, 3, 15, 1)

    with jax.named_scope("tokens"):
        for t in range(2):
            own_tok[t].wait()
            block = xs.at[t, own8, :]
            for k in all_far:
                send(block, block, xsem.at[0], xsem.at[1 + t], at_gy(lax.rem(h + k, NG)))

    def tokens_in(t):
        arrived(xs.at[t, pl.ds(0, 120), :], xsem.at[1 + t])

    slots = {}

    def slot_of(tq):
        slots[tq] = slots.get(tq, -1) + 1
        return slots[tq]

    def enc(q, v):
        return encode4(v) if q < 2 else encode2(v)

    def dec(q, v):
        return decode4(v) if q < 2 else decode2(v)

    def long_way(q, t):
        return (q + t) % 2

    def chunk(t, q, d, k):
        return part[t, q, zat(way(d, k))]

    def send_whole(t, q, val, d, hops, slot):
        tq = t
        i = slot_of(tq)
        sbuf[tq, i] = enc(q, val)
        send(sbuf.at[tq, i], rbuf.at[tq, d, slot], rss, rsr.at[tq, d, slot], column(way(d, hops)))

    def send_last(t, q, val, d, hops, slot):
        tq = t
        i = slot_of(tq)
        sbuf[tq, i] = enc(q, val)
        for other in (True, False):
            y = 1 - yh if other else yh
            dst = fin.at[tq, slot + d + (2 if other else 0)]
            send(sbuf.at[tq, i, y], dst, rss, fsr.at[tq], column(way(d, hops), other))

    def send_pair(t, q):
        tq = t
        pbuf[tq] = enc(q, part[t, q, z, 1 - yh])
        send(pbuf.at[tq], fin.at[tq, 4], pss, fsr.at[tq], column(0, True))

    def taken(t, q, d, slot):
        tq = t
        arrived(rbuf.at[tq, d, slot], rsr.at[tq, d, slot])
        return dec(q, rbuf[tq, d, slot])

    def total(t, q, n):
        tq = t
        arrived(fin.at[tq, pl.ds(0, n)], fsr.at[tq])
        val = part[t, q, z, yh]
        for i in range(n):
            val = val + dec(q, fin[tq, i])
        return val

    def up(t, q):
        for u in range(2):
            for n in range(0, FL, 256):
                m = min(256, FL - n)
                val = jnp.dot(xs[t], wup[2 * q + u, :, n : n + m], preferred_element_type=F32)
                part[t, q, :, :, u, :, n : n + m] = val.reshape(8, 2, 8, m)

    def ring_start(t):
        d = long_way(0, t)
        send_whole(t, 0, chunk(t, 0, d, 4), d, 1, 0)
        send_whole(t, 0, chunk(t, 0, 1 - d, 3), 1 - d, 1, 1)
        send_pair(t, 0)

    def ring(t, q, d, s):
        val = chunk(t, q, d, 4 - s) + taken(t, q, d, s - 1)
        if s < 3:
            send_whole(t, q, val, d, 1, s)
        else:
            send_last(t, q, val, d, 1, 0)

    waited = set()

    def cross_group(i):
        return {4: 0, 3: 0, 5: 0, 2: 1, 6: 1}.get(i, 2)

    def cross(t, ks):
        d = long_way(1, t)
        for k in ks:
            i = way(d, k) % NZ
            ysb[t, i] = enc(0, part[t, 1, zat(i), 1 - yh])
            send(ysb.at[t, i], yrb.at[t, i], yss, ysr.at[t, cross_group(i)], column(0, True))

    def crossed(t, k):
        i = k % NZ
        e = cross_group(i)
        if (t, e) not in waited:
            waited.add((t, e))
            arrived(yrb.at[t, pl.ds(0, 2 if e == 1 else 3)], ysr.at[t, e])
        return part[t, 1, zat(i), yh] + dec(0, yrb[t, i])

    def half_ring(t, d, s):
        val = crossed(t, way(d, 4 - s))
        first = 0 if d == long_way(1, t) else 1
        if s > first:
            arrived(hrb.at[t, d, s - 1], hsr.at[t, d, s - 1])
            val = val + dec(0, hrb[t, d, s - 1])
        i = slot_of(10 + t)
        hsb[t, i] = enc(0, val)
        send(hsb.at[t, i], hrb.at[t, d, s], hss, hsr.at[t, d, s], column(way(d, 1)))

    def half_total(t):
        val = crossed(t, 0)
        for d in range(2):
            arrived(hrb.at[t, d, 3], hsr.at[t, d, 3])
            val = val + dec(0, hrb[t, d, 3])
        return val

    def group(e, t, rows):
        return ag.at[e // 2, pl.ds(0, 2) if e == 2 else pl.ds(e, 1), t, rows, :]

    def gather(e, t):
        own = group(e, t, zown)
        for k, slot in ((2, 0), (1, 2)):
            for d in range(2):
                for other in (True, False):
                    send(own, own, ags, agr.at[t, e, d if k == 2 else 2], column(way(d, k), other))
        send(own, own, ags, agr.at[t, e, 2], column(0, True))

    def relay(e, t, d):
        arrived(group(e, t, pl.ds(0, 16)), agr.at[t, e, d])
        rows = group(e, t, pl.ds(pl.multiple_of(16 * zat(way(d, -2)), 16), 16))
        if d == long_way(e, t):
            send(rows, rows, ags, agr.at[t, e, 2], column(way(d, 2)))
        send(rows, rows, ags, agr.at[t, e, 2], column(way(d, 1)))

    def gathered(e, t):
        arrived(group(e, t, pl.ds(0, 88)), agr.at[t, e, 2])

    def hidden_value(t):
        val = total(t, 0, 5)
        act[t, 0] = val[0]
        act[t, 1] = val[1]
        ag[0, 0, t, zown, :] = (silu_parts(val[0])[0] * val[1]).astype(BF16)
        gather(0, t)

    def hidden_tangent(t):
        val = half_total(t)
        gate, upper, gate_dot, upper_dot = act[t, 0], act[t, 1], val[0], val[1]
        silu_val, first, second = silu_parts(gate)
        ag[0, 1, t, zown, :] = (first * gate_dot * upper + silu_val * upper_dot).astype(BF16)
        gather(1, t)
        act[t, 2] = gate_dot
        act[t, 3] = upper_dot

    def out(t, w):
        gathered(w, t)
        for n in range(0, DL, 256):
            cols = slice(n, n + 256)
            val = jnp.dot(ag[0, w, t], wdn[0, :, cols], preferred_element_type=F32)
            if w == 1:
                val = val + jnp.dot(ag[0, 0, t], wdn[1, :, cols], preferred_element_type=F32)
            osum[t, w, :, :, :, cols] = val.reshape(2, 8, 8, 256)
        osend[t, w] = encode2(osum[t, w, 1 - core])
        send(osend.at[t, w], ocore.at[t, w], oss.at[0], osr.at[0, t, w], at_gy(mate))

    def out_send(t, w):
        arrived(ocore.at[t, w], osr.at[0, t, w])
        val = osum[t, w, core] + decode2(ocore[t, w])
        osum[t, w, core] = val
        oown[t, w] = encode2(val)
        for k in far:
            dst = lax.rem(mine + k, 8)
            send(oown.at[t, w, dst], orecv.at[t, w, k], oss.at[1], osr.at[1, t, w], at_gy(2 * dst + core))

    def grads(t, w):
        arrived(orecv.at[t, w, pl.ds(1, 7)], osr.at[1, t, w])
        val = osum[t, w, core, mine]
        for k in range(1, 8):
            val = val + decode2(orecv[t, w, k])
        if w == 0:
            val = val - tgv[8 * t : 8 * t + 8, :].astype(F32)
        gs[t, w, own8, :] = (val * scale).astype(BF16)
        own = gs.at[t, w, own8, :]
        for k in all_far:
            send(own, own, gss, gsr.at[t, w], at_gy(lax.rem(h + k, NG)))

    def back(t, u):
        arrived(gs.at[t, u, pl.ds(0, 120), :], gsr.at[t, u])
        for n in range(0, FL, 256):
            m = min(256, FL - n)
            val = tail_dot(gs[t, u], wdn[0, n : n + m, :])
            if u == 1:
                val = val + tail_dot(gs[t, 0], wdn[1, n : n + m, :])
            part[t, 2, :, :, u, :, n : n + m] = val.reshape(8, 2, 8, m)
        for d in range(2):
            back_far(t, u, d, 3, 1, 0)
        back_far(t, u, (t + u) % 2, 4, 2, 1)
        for d in range(2):
            back_last(t, u, d, 1, part[t, 2, zat(way(d, 1)), :, u], 0)
        bpb[t, u] = encode2(part[t, 2, z, 1 - yh, u])
        send(bpb.at[t, u], bfin.at[t, u, 4], bpb_sem, bfin_sem.at[t, u], column(0, True))

    def back_far(t, u, d, k, hops, slot):
        i = slot_of((t, u))
        bsb[t, u, i] = encode2(part[t, 2, zat(way(d, k)), :, u])
        send(bsb.at[t, u, i], brb.at[t, u, d, slot], bsb_sem, brb_sem.at[t, u, 2 if slot else d], column(way(d, hops)))

    def back_last(t, u, d, k, val, slot):
        i = slot_of((t, u))
        bsb[t, u, i] = encode2(val)
        for other in (True, False):
            y = 1 - yh if other else yh
            dst = bfin.at[t, u, slot + d + (2 if other else 0)]
            send(bsb.at[t, u, i, y], dst, bsb_sem, bfin_sem.at[t, u], column(way(d, k), other))

    def fold(t, u, d):
        val = part[t, 2, zat(way(d, 2)), :, u]
        for slot in range(2 if d == (t + u) % 2 else 1):
            arrived(brb.at[t, u, d, slot], brb_sem.at[t, u, 2 if slot else d])
            val = val + decode2(brb[t, u, d, slot])
        back_last(t, u, d, 2, val, 5)

    def summed(t, u):
        arrived(bfin.at[t, u], bfin_sem.at[t, u])
        val = part[t, 2, z, yh, u]
        for i in range(9):
            val = val + decode2(bfin[t, u, i])
        return val

    def inner(t):
        back_val, back_dot = summed(t, 0), summed(t, 1)
        gate, upper, gate_dot, upper_dot = act[t, 0], act[t, 1], act[t, 2], act[t, 3]
        silu_val, first, second = silu_parts(gate)
        ag[1, 0, t, zown, :] = (
            back_dot * upper * first + back_val * upper_dot * first + back_val * upper * second * gate_dot
        ).astype(BF16)
        ag[1, 1, t, zown, :] = (back_dot * silu_val + back_val * first * gate_dot).astype(BF16)
        gather(2, t)

    def down(n):
        g0 = gs[:, 0, :, n : n + 256].reshape(TOKENS, 256)
        g1 = gs[:, 1, :, n : n + 256].reshape(TOKENS, 256)
        hid = ag[0, 0].reshape(TOKENS, FL)
        hid_dot = ag[0, 1].reshape(TOKENS, FL)
        hd[:, n : n + 256] = (lead_dot(hid_dot, g0) + lead_dot(hid, g1)).astype(BF16)

    def flat(t):
        xt[:, 128 * t : 128 * t + 128] = xs[t].T

    def both(f, *a):
        for d in range(2):
            f(*a, d)

    def up_waited(t, q):
        if t == 0:
            local[2 * q].wait()
            local[2 * q + 1].wait()
        if q == 1:
            tokens_in(t)
        up(t, q)

    def out_waited(t, w):
        if t == 0:
            local[4 + w].wait()
        if t == 0 and w == 0:
            own_tgt.wait()
        out(t, w)

    def half_way(t, short, s):
        half_ring(t, (long_way(1, t) + short) % 2, s)

    def full_way(t, short, s):
        ring(t, 0, (long_way(0, t) + short) % 2, s)

    steps = {
        "up": up_waited,
        "cross0": lambda t: cross(t, (4, -3, 3)),
        "cross1": lambda t: cross(t, (2, -2, 1, -1, 0)),
        "start": ring_start,
        "half": half_way,
        "full": full_way,
        "hidden": hidden_value,
        "hiddent": hidden_tangent,
        "pass": lambda t: both(relay, 0, t),
        "passt": lambda t: both(relay, 1, t),
        "out": out_waited,
        "outs": out_send,
        "grads": grads,
        "back": back,
        "fold": lambda t, u: both(fold, t, u),
        "inner": inner,
        "pass1": lambda t: both(relay, 2, t),
        "down": down,
        "flat": flat,
    }
    for name, *a in ORDER:
        with jax.named_scope(name + "_".join(str(i) for i in a)):
            steps[name](*a)
    xt_copy = local_copy(xt, xt_out, 2)
    hd_copy = local_copy(hd, hd_out, 3)
    ag_copies = []
    for t in range(2):
        with jax.named_scope("gathered%d" % t):
            gathered(2, t)
            ag_copies.append(local_copy(ag.at[1, :, t], ag_out.at[:, t], t))
    with jax.named_scope("tail"):
        left(xs.at[:, pl.ds(0, 120), :], xsem.at[0])
        left(sbuf, rss)
        left(pbuf, pss)
        left(ysb, yss)
        left(hsb, hss)
        left(bsb, bsb_sem)
        left(bpb, bpb_sem)
        left(ag.at[:, :, :, pl.ds(0, 120), :], ags)
        left(osend, oss.at[0])
        left(oown.at[:, :, pl.ds(0, 7)], oss.at[1])
        left(gs.at[:, :, pl.ds(0, 120), :], gss)
        xt_copy.wait()
        hd_copy.wait()
        for c in ag_copies:
            c.wait()


def weights_kernel(xt, ag, hd, gate_out, up_out, down_out, buf, sem):
    rows = DL // 4
    down = pltpu.make_async_copy(hd, down_out, sem.at[8])
    down.start()
    copies = []
    for v, out in enumerate((gate_out, up_out)):
        for i in range(4):
            part = pl.ds(i * rows, rows)
            buf[v, part, :] = jnp.dot(xt[part, :], ag[v], preferred_element_type=F32).astype(BF16)
            copy = pltpu.make_async_copy(buf.at[v, part, :], out.at[part, :], sem.at[4 * v + i])
            copy.start()
            copies.append(copy)
    down.wait()
    for copy in copies:
        copy.wait()


def body(*args):
    hbm = pl.BlockSpec(memory_space=pltpu.HBM)
    vmem = pl.BlockSpec(memory_space=pltpu.VMEM)
    dma = pltpu.SemaphoreType.DMA
    args = [pltpu.with_memory_space_constraint(a, pltpu.HBM) for a in args]
    xt, ag, hd = pl.pallas_call(
        kernel,
        out_shape=(
            jax.ShapeDtypeStruct((DL, TOKENS), BF16),
            jax.ShapeDtypeStruct((2, 2, 128, FL), BF16),
            jax.ShapeDtypeStruct((FL, DL), BF16),
        ),
        in_specs=[hbm] * 8,
        out_specs=(pl.BlockSpec(memory_space=pl.ANY),) * 3,
        scratch_shapes=[
            pltpu.VMEM((2, 128, DL), BF16),
            pltpu.VMEM((DL, TOKENS), BF16),
            pltpu.VMEM((FL, DL), BF16),
            pltpu.VMEM((TOKENS // NG, DL), BF16),
            pltpu.VMEM((4, DL, FL), BF16),
            pltpu.VMEM((2, FL, DL), BF16),
            pltpu.VMEM((2, 3, 8, 2, 2, 8, FL), F32),
            pltpu.VMEM((2, 7, 2, 2, 8, FL), BF16),
            pltpu.VMEM((2, 2, 3, 2, 2, 8, FL), BF16),
            pltpu.VMEM((2, 2, 8, FL), BF16),
            pltpu.VMEM((2, 5, 2, 8, FL), BF16),
            pltpu.VMEM((2, 8, 2, 8, FL), BF16),
            pltpu.VMEM((2, 8, 2, 8, FL), BF16),
            pltpu.VMEM((2, 7, 2, 8, FL), BF16),
            pltpu.VMEM((2, 2, 4, 2, 8, FL), BF16),
            pltpu.VMEM((2, 2, 7, 2, 8, FL), BF16),
            pltpu.VMEM((2, 2, 2, 2, 2, 8, FL), BF16),
            pltpu.VMEM((2, 2, 8, FL), BF16),
            pltpu.VMEM((2, 2, 9, 8, FL), BF16),
            pltpu.VMEM((2, 4, 8, FL), F32),
            pltpu.VMEM((2, 2, 2, 128, FL), BF16),
            pltpu.VMEM((2, 2, 2, 8, 8, DL), F32),
            pltpu.VMEM((2, 2, 8, 8, DL), BF16),
            pltpu.VMEM((2, 2, 8, 8, DL), BF16),
            pltpu.VMEM((2, 2, 8, 8, DL), BF16),
            pltpu.VMEM((2, 2, 8, 8, DL), BF16),
            pltpu.VMEM((2, 2, 128, DL), BF16),
            dma((9,)),
            dma((3,)),
            dma, dma,
            dma((2, 2, 3)),
            dma((2,)),
            dma, dma((2, 3)),
            dma, dma((2, 2, 4)),
            dma, dma((2, 2, 3)), dma, dma((2, 2)),
            dma,
            dma((2, 3, 3)),
            dma((2,)), dma((2, 2, 2)),
            dma, dma((2, 2)),
        ],
        compiler_params=pltpu.CompilerParams(
            collective_id=0, has_side_effects=True, vmem_limit_bytes=40 * 1024 * 1024
        ),
    )(*args)
    return pl.pallas_call(
        weights_kernel,
        out_shape=(
            jax.ShapeDtypeStruct((DL, FL), BF16),
            jax.ShapeDtypeStruct((DL, FL), BF16),
            jax.ShapeDtypeStruct((FL, DL), BF16),
        ),
        in_specs=[vmem] * 3,
        out_specs=(hbm,) * 3,
        scratch_shapes=[pltpu.VMEM((2, DL, FL), BF16), dma((9,))],
        compiler_params=pltpu.CompilerParams(vmem_limit_bytes=16 * 1024 * 1024),
    )(xt, ag.reshape(2, TOKENS, FL), hd)


def solution(mesh):
    in_specs = (
        P("gy", "gx"),
        P("gy", "gx"),
        P("gx", "gy"),
        P("gx", "gy"),
        P("gy", "gx"),
        P("gx", "gy"),
        P("gx", "gy"),
        P("gy", "gx"),
    )
    out_specs = (P("gx", "gy"), P("gx", "gy"), P("gy", "gx"))
    return jax.shard_map(body, mesh=mesh, in_specs=in_specs, out_specs=out_specs, check_vma=False)
```
